512 devices in a mesh: grp: 2 (over y), sp: 128 (over x, z), ch: 2 (over core).
Axes of the slice: x: 4, y: 2, z: 32, core: 2. Of those that a mesh axis runs over, the one named last changes fastest.
The devices are a block of a 4x8x32 slice.
Arguments:
- latents: bfloat16 [262144, 1024], P(('grp', 'sp')), parts along dimension 0, may hold values from -6 to 6
- spectrum: bfloat16 [16, 64, 128, 1024], P(None, None, 'sp', 'ch'), may hold values from -4 to 4
- w_value: bfloat16 [1024, 1024], P('sp', 'ch'), may hold values from -0.1875 to 0.1875
- w_gate: bfloat16 [1024, 1024], P('sp', 'ch'), may hold values from -0.1875 to 0.1875
- w_out: bfloat16 [1024, 1024], P('sp'), may hold values from -0.1875 to 0.1875
- embed_table: bfloat16 [1024, 32768], P(('sp', 'ch')), may hold values from -12 to 12
- prompt_ids: int32 [512], P('grp'), parts along dimension 0, may hold values from 0 to 32767
- noise_step: int32 [2], P('grp'), parts along dimension 0, may hold values from 0 to 999
Outputs:
- denoised: bfloat16 [262144, 1024], P(('grp', 'sp', 'ch')), parts along dimension 0
The draws below stay inside these ranges and needn't reach their ends.
There are 2 independent parts, one for each index of `grp`. The reference program is written for one: setup_inputs(seed, part) draws one part's arguments, and reference() takes and returns one part's arrays. A program takes and returns all parts, laid end to end along the dimension named above; an argument that names none is the same for every part. Nothing has to cross between parts.
All inputs are finite; a program needn't handle non-finite values.
Results may differ from the reference program's by a relative error of at most 0.013.
Values may be sent and summed in bfloat16 or wider, within the bound.
A program may use at most 64 MiB of HBM per device.

```python
import math
import jax
import jax.numpy as jnp
import numpy as np
from jax import lax

TT = 16
HH = 64
WW = 128
C = 1024
VOCAB = 32768
PROMPT = 256
CELLS = 131072


def plant(drawn, own_key, low, high):
    longest = drawn.shape.index(max(drawn.shape))
    spots = []
    for shift in (0, 1):
        where = [jax.random.randint(jax.random.fold_in(own_key, axis), (), 0, length) for axis, length in enumerate(drawn.shape)]
        where[longest] = (where[longest] + shift) % drawn.shape[longest]
        spots.append(tuple(where))
    return drawn.at[spots[0]].set(low).at[spots[1]].set(high)


def shard_levels(key, dims, cuts, least, top_value):
    loudness, own = 1.0, jax.random.fold_in(key, 6)
    for axis_at, shards_of in cuts:
        draws = jnp.exp(jax.random.uniform(jax.random.fold_in(own, axis_at), (shards_of,), jnp.float32, least / len(cuts), top_value / len(cuts)))
        loudness = loudness * jnp.repeat(draws, dims[axis_at] // shards_of).reshape([-1 if axis == axis_at else 1 for axis in range(len(dims))])
    return loudness


def rank_table(amount, slope):
    weights = [(1 << 20) // math.isqrt(grade ** slope) + 1 for grade in range(1, amount + 1)]
    width = 1 + sum(weights) // (1 << 30)
    return np.cumsum(np.array([max(1, weight // width) for weight in weights]))


def ranked(key, dims, count, lean):
    table = rank_table(count, lean)
    lot = jax.random.randint(jax.random.fold_in(key, 1), dims, 0, int(table[count - 1]))
    rank = jnp.searchsorted(jnp.asarray(table, jnp.int32), lot, side="right")
    return jax.random.permutation(jax.random.fold_in(key, 2), count)[rank].astype(jnp.int32)


def bell_draw(own_key, dims, scale, limit, cuts=(), held_as=jnp.bfloat16):
    values = scale * jax.random.normal(own_key, dims, jnp.float32)
    if cuts:
        values = values * shard_levels(own_key, dims, cuts, -0.22, 0.18)
    return jnp.clip(values, -limit, limit).astype(held_as)


def setup_inputs(seed: int = 0, part: int = 0) -> dict:
    key_list = jax.random.split(jax.random.key(seed), 9)
    part_keys = jax.random.split(jax.random.fold_in(key_list[8], part), 9)
    latents = bell_draw(part_keys[0], (CELLS, C), 1.0, 6.0, ((0, 128),))
    spectrum = bell_draw(key_list[1], (TT, HH, WW, C), 1.0, 4.0, ((2, 128), (3, 2)))
    w_value = bell_draw(key_list[2], (C, C), C ** -0.5, 0.1875, ((0, 128), (1, 2)))
    w_gate = bell_draw(key_list[3], (C, C), C ** -0.5, 0.1875, ((0, 128), (1, 2)))
    w_out = bell_draw(key_list[4], (C, C), C ** -0.5, 0.1875, ((0, 128),))
    embed_table = bell_draw(key_list[5], (C, VOCAB), 3.0, 12.0, ((0, 256),))
    prompt_ids = plant(ranked(part_keys[6], (PROMPT,), VOCAB, 2), jax.random.fold_in(part_keys[6], 3), 0, VOCAB - 1).astype(jnp.int32)
    noise_step = jax.random.randint(part_keys[7], (1,), 0, 1000).astype(jnp.int32)
    return {"latents": latents, "spectrum": spectrum, "w_value": w_value, "w_gate": w_gate, "w_out": w_out, "embed_table": embed_table, "prompt_ids": prompt_ids, "noise_step": noise_step}


def cas_table(length):
    position = jnp.arange(length, dtype=jnp.int32)
    product = position[:, None] * position[None, :] % length
    phase_angle = product.astype(jnp.float32) * (2.0 * math.pi / length)
    return ((jnp.cos(phase_angle) + jnp.sin(phase_angle)) / math.sqrt(length)).astype(jnp.bfloat16)

def step_embedding(noise_step, channel, channels):
    half_count = channels // 2
    lower_half = channel < half_count
    position = jnp.where(lower_half, channel, channel - half_count).astype(jnp.float32)
    frequency = jnp.exp(-math.log(10000.0) * position / half_count)
    phase_angle = noise_step[0].astype(jnp.float32) * frequency
    return jnp.where(lower_half, jnp.sin(phase_angle), jnp.cos(phase_angle))

def apply_table(form, table, operand):
    return jnp.einsum(form, table.astype(jnp.float32), operand.astype(jnp.float32), precision=lax.Precision.HIGHEST)

def reference(latents, spectrum, w_value, w_gate, w_out, embed_table, prompt_ids, noise_step):
    channel = jnp.arange(C, dtype=jnp.int32)
    pooled = lax.optimization_barrier(jnp.mean(jnp.take(embed_table, prompt_ids, axis=1).astype(jnp.float32), axis=1))
    modulation = 1.0 + pooled + step_embedding(noise_step, channel, C)
    value_rows = jnp.dot(latents, w_value, preferred_element_type=jnp.float32).astype(jnp.bfloat16)
    gate_rows = jnp.dot(latents, w_gate, preferred_element_type=jnp.float32)
    cas_width = cas_table(WW)
    cas_height = cas_table(HH)
    cas_time = cas_table(TT)
    latent_grid = value_rows.reshape(TT, HH, WW, C)
    width_spec = apply_table('kw,thwc->thkc', cas_width, latent_grid).astype(jnp.bfloat16)
    height_spec = apply_table('ah,thkc->takc', cas_height, width_spec).astype(jnp.bfloat16)
    full_spec = apply_table('st,takc->sakc', cas_time, height_spec).astype(jnp.bfloat16)
    filtered = (full_spec.astype(jnp.float32) * spectrum.astype(jnp.float32)).astype(jnp.bfloat16)
    time_back = apply_table('ts,sakc->takc', cas_time, filtered).astype(jnp.bfloat16)
    height_back = apply_table('ha,takc->thkc', cas_height, time_back).astype(jnp.bfloat16)
    mix_rows = apply_table('wk,thkc->thwc', cas_width, height_back).reshape(TT * HH * WW, C)
    mixed_rows = (mix_rows * jax.nn.silu(gate_rows) * modulation[None, :]).astype(jnp.bfloat16)
    projected = jnp.dot(mixed_rows, w_out, preferred_element_type=jnp.float32)
    return (latents.astype(jnp.float32) + projected).astype(jnp.bfloat16)
```

```python
import math

import jax
import jax.numpy as jnp
from jax import lax
from jax.sharding import Mesh
from jax.sharding import PartitionSpec as P

TT = 16
HH = 64
WW = 128
C = 1024
SP = ("sp_0", "sp_1")
SP_CH = ("sp_0", "sp_1", "ch")
GRP_SP = ("grp", "sp_0", "sp_1")
GRP_SP_CH = ("grp", "sp_0", "sp_1", "ch")
F32 = jnp.float32
BF16 = jnp.bfloat16


def cas_table(length):
    position = jnp.arange(length, dtype=jnp.int32)
    product = position[:, None] * position[None, :] % length
    phase_angle = product.astype(jnp.float32) * (2.0 * math.pi / length)
    return ((jnp.cos(phase_angle) + jnp.sin(phase_angle)) / math.sqrt(length)).astype(jnp.bfloat16)


def step_embedding(noise_step, channel, channels):
    half_count = channels // 2
    lower_half = channel < half_count
    position = jnp.where(lower_half, channel, channel - half_count).astype(jnp.float32)
    frequency = jnp.exp(-math.log(10000.0) * position / half_count)
    phase_angle = noise_step[0].astype(jnp.float32) * frequency
    return jnp.where(lower_half, jnp.sin(phase_angle), jnp.cos(phase_angle))


def dot(a, b):
    return jnp.dot(a, b, preferred_element_type=F32)


def local_pool(embed_table, prompt_ids):
    vocab = embed_table.shape[1]
    low = 256
    high_hot = (prompt_ids[:, None] // low == jnp.arange(vocab // low)[None, :]).astype(BF16)
    low_hot = (prompt_ids[:, None] % low == jnp.arange(low)[None, :]).astype(BF16)
    counts = jnp.einsum("ph,pl->hl", high_hot, low_hot, preferred_element_type=F32)
    total = jnp.sum(embed_table.astype(F32) * counts.reshape(1, vocab), axis=1)
    return total / prompt_ids.shape[0]


def local(latents, spectrum, w_value, w_gate, w_out, embed_table, prompt_ids, noise_step):
    row_count = latents.shape[0]
    part = w_value.shape[1]
    lines = row_count // WW
    core = lax.axis_index("ch")
    offset = core * part

    pool4 = local_pool(embed_table, prompt_ids)
    pool8 = lax.all_gather(pool4, "ch", axis=0, tiled=True)
    high = lax.reduce_precision(pool8, 8, 7)
    low = pool8 - high
    pool_cols = jnp.pad(jnp.stack([high, low], axis=1), ((0, 0), (0, 126))).astype(BF16)
    packed = jnp.concatenate([w_value, w_gate, w_out, pool_cols], axis=1)
    column = lax.all_gather(packed, "sp_1", axis=0, tiled=True)
    weights = lax.all_gather(column, "sp_0", axis=0, tiled=True)

    cas_width = cas_table(WW)
    space = jnp.einsum("st,ah->sath", cas_table(TT).astype(F32), cas_table(HH).astype(F32))
    space = space.reshape(TT * HH, TT * HH).astype(BF16)

    mine = lax.dynamic_slice_in_dim(latents, offset, part, 1).reshape(lines, WW, part)
    spread = jnp.einsum("kw,lwc->klc", cas_width, mine, preferred_element_type=F32).astype(BF16)
    arrived = lax.all_to_all(spread, SP, split_axis=0, concat_axis=0, tiled=True)
    arrived = arrived.reshape(TT * HH, part)
    both = lax.all_gather(arrived, "ch", axis=1, tiled=True)
    width_spec = dot(both, weights[:, :part]).astype(BF16)
    full_spec = dot(space, width_spec).astype(BF16)
    gains = spectrum.reshape(TT * HH, part)
    filtered = (full_spec.astype(F32) * gains.astype(F32)).astype(BF16)
    height_back = dot(space, filtered).astype(BF16)
    returned = lax.all_to_all(
        height_back.reshape(-1, lines, part), SP, split_axis=0, concat_axis=0, tiled=True
    )
    gate_rows = dot(latents, weights[:, part : 2 * part])
    pooled_all = weights[:, 2 * part + C].astype(F32) + weights[:, 2 * part + C + 1].astype(F32)
    pooled = lax.dynamic_slice_in_dim(pooled_all, offset, part)
    channel = offset + jnp.arange(part, dtype=jnp.int32)
    modulation = 1.0 + pooled + step_embedding(noise_step, channel, C)
    gain = jax.nn.silu(gate_rows) * modulation[None, :]
    mix_rows = jnp.einsum("wk,klc->lwc", cas_width, returned, preferred_element_type=F32)
    mixed = (mix_rows.reshape(row_count, part) * gain).astype(BF16)
    half = row_count // lax.axis_size("ch")
    moved = lax.all_to_all(mixed, "ch", split_axis=0, concat_axis=1, tiled=True)
    summed = dot(moved, weights[:, 2 * part : 2 * part + C])
    residual = lax.dynamic_slice_in_dim(latents, core * half, half, 0)
    return (residual.astype(F32) + summed).astype(BF16)


def solution(mesh):
    torus = Mesh(
        mesh.devices.reshape(mesh.shape["grp"], 4, 32, mesh.shape["ch"]),
        ("grp", "sp_0", "sp_1", "ch"),
    )
    in_specs = (
        P(GRP_SP, None),
        P(None, None, SP, "ch"),
        P(SP, "ch"),
        P(SP, "ch"),
        P(SP, None),
        P(SP_CH, None),
        P("grp"),
        P("grp"),
    )
    out_specs = P(GRP_SP_CH, None)
    return jax.shard_map(local, mesh=torus, in_specs=in_specs, out_specs=out_specs, check_vma=False)
```

```python
import functools
import math

import jax
import jax.numpy as jnp
import numpy as np
from jax import lax
from jax.experimental import pallas as pl
from jax.experimental.pallas import tpu as pltpu
from jax.sharding import Mesh
from jax.sharding import PartitionSpec as P

TT = 16
HH = 64
WW = 128
SP_CH = ("sp_0", "sp_1", "ch")
GRP_SP = ("grp", "sp_0", "sp_1")
GRP_SP_CH = ("grp", "sp_0", "sp_1", "ch")
SP = ("sp_0", "sp_1")
F32 = jnp.float32
BF16 = jnp.bfloat16
MESH = pl.DeviceIdType.MESH
STRIDE = 4
WINDOW = 16


def cas_table(length):
    position = np.arange(length, dtype=np.int32)
    product = position[:, None] * position[None, :] % length
    phase_angle = product.astype(np.float32) * np.float32(2.0 * math.pi / length)
    table = (np.cos(phase_angle) + np.sin(phase_angle)) / np.float32(math.sqrt(length))
    return jnp.asarray(table.astype(jnp.bfloat16))


def step_embedding(noise_step, channel, channels):
    half_count = channels // 2
    lower_half = channel < half_count
    position = jnp.where(lower_half, channel, channel - half_count).astype(jnp.float32)
    frequency = jnp.exp(-math.log(10000.0) * position / half_count)
    phase_angle = noise_step[0].astype(jnp.float32) * frequency
    return jnp.where(lower_half, jnp.sin(phase_angle), jnp.cos(phase_angle))


def dot(a, b):
    return jnp.dot(a, b, preferred_element_type=F32)


def iota(shape, dim):
    return lax.broadcasted_iota(jnp.int32, shape, dim)


def one_hot(condition):
    return jnp.where(condition, 1.0, 0.0).astype(BF16)


def kernel(
    nx, nz,
    lat, spec, wv_in, wg_in, wo_in, table, ids, emb, kw, kh, kt,
    out,
    spread, arrived, spin, spout, back, returned, y_own, y_other, filt, gain,
    wv, wgo, wo_other, mix_own, mix_other, counts, space, wide, narrow,
    a_send, a_recv, b_send, b_recv, s_send, s_recv, r_send, r_recv, x_send, x_recv,
    y_send, y_recv, o_send, o_recv, m_send, m_recv,
):
    n = nx * nz
    rows, chans = lat.shape
    part = wv_in.shape[1]
    lines = rows // WW
    block = rows // n
    mx, mz, core = lax.axis_index("sp_0"), lax.axis_index("sp_1"), lax.axis_index("ch")
    me = mx * nz + mz
    other_core = {"ch": 1 - core}

    def partner(i):
        j = n - 1 - i
        zi, dx = j // nx, j % nx
        m = (zi + 1) // 2
        dz = jnp.where(zi % 2 == 1, m, nz - m) % nz
        tx, tz = (mx + dx) % nx, (mz + dz) % nz
        return {"sp_0": tx, "sp_1": tz}, tx * nz + tz

    barrier = pltpu.get_barrier_semaphore()

    def greet(i, carry):
        device, _ = partner(i)
        pl.semaphore_signal(barrier, inc=1, device_id=device, device_id_type=MESH)
        return carry

    lax.fori_loop(0, n - 1, greet, 0)
    pl.semaphore_signal(barrier, inc=1, device_id=other_core, device_id_type=MESH)

    pick = one_hot(iota((rows, WW), 0) // lines == iota((rows, WW), 1))
    spread_rows = dot(pick, kw[...]).astype(BF16)
    line_of = iota((rows, WW), 0) % lines
    for line in range(lines):
        narrow[:, line * WW : (line + 1) * WW] = jnp.where(
            line_of == line, spread_rows, jnp.zeros_like(spread_rows)
        )
    mine = pl.ds(pl.multiple_of(core * part, 128), part)
    tile = 256
    per = tile // block

    def widen(r, carry):
        at = pl.ds(pl.multiple_of(r * tile, tile), tile)
        got = dot(narrow[at, :], lat[:, mine]).astype(BF16)
        spread[pl.ds(r * per, per)] = got.reshape(per, block, part)
        return carry

    lax.fori_loop(0, rows // tile, widen, 0)
    arrived[me] = spread[me]
    wv[mx, mz // STRIDE, mz % STRIDE] = wv_in[...]
    wgo[mx, mz // STRIDE, mz % STRIDE, :, 0:part] = wg_in[...]
    wgo[mx, mz // STRIDE, mz % STRIDE, :, part : 2 * part] = wo_in[:, mine]

    pl.semaphore_wait(barrier, n)

    groups = nz // STRIDE
    up = (groups + 1) // 2
    down = groups - 1 - up

    def hop(stream, direction, q):
        buf = (wv, wgo)[stream]
        origin = (mz // STRIDE - direction * (q - 1) + groups) % groups
        ref = buf.at[mx, origin, mz % STRIDE]
        k = (q - 1) if direction > 0 else up + q - 1
        return pltpu.make_async_remote_copy(
            src_ref=ref, dst_ref=ref,
            send_sem=s_send.at[stream, k], recv_sem=s_recv.at[stream, k],
            device_id={"sp_1": (mz + direction * STRIDE + nz) % nz}, device_id_type=MESH,
        )

    def near(stream, k):
        buf = (wv, wgo)[stream]
        ref = buf.at[mx, :, mz % STRIDE]
        step = (1, -1, 2)[k]
        return pltpu.make_async_remote_copy(
            src_ref=ref, dst_ref=ref,
            send_sem=r_send.at[stream, k], recv_sem=r_recv.at[stream, k],
            device_id={"sp_1": (mz + step + nz) % nz}, device_id_type=MESH,
        )

    def across(stream, k):
        buf = (wv, wgo)[stream]
        ref = buf.at[mx]
        return pltpu.make_async_remote_copy(
            src_ref=ref, dst_ref=ref,
            send_sem=x_send.at[stream, k], recv_sem=x_recv.at[stream, k],
            device_id={"sp_0": (mx + k + 1) % nx}, device_id_type=MESH,
        )

    def near_in(stream, k):
        buf = (wv, wgo)[stream]
        step = (1, -1, 2)[k]
        ref = buf.at[mx, :, (mz - step + nz) % STRIDE]
        return pltpu.make_async_copy(ref, ref, r_recv.at[stream, k])

    def gather_step(stream, step):
        if 0 < step <= up:
            hop(stream, 1, step).wait_recv()
        if 0 < step <= down:
            hop(stream, -1, step).wait_recv()
        if step < up:
            hop(stream, 1, step + 1).start()
        if step < down:
            hop(stream, -1, step + 1).start()
        if step == up:
            for k in range(3):
                near(stream, k).start()
        if step == up + 1:
            for k in range(3):
                near_in(stream, k).wait()
            for k in range(nx - 1):
                across(stream, k).start()
        if step == up + 2:
            for k in range(nx - 1):
                across(stream, k).wait_recv()
            for q in range(up):
                hop(stream, 1, q + 1).wait_send()
            for q in range(down):
                hop(stream, -1, q + 1).wait_send()
            for k in range(3):
                near(stream, k).wait_send()
            for k in range(nx - 1):
                across(stream, k).wait_send()

    def exchange(src, dst, send_sem, recv_sem):
        def copy(i):
            device, target = partner(i)
            return pltpu.make_async_remote_copy(
                src_ref=src.at[target], dst_ref=dst.at[me],
                send_sem=send_sem.at[i], recv_sem=recv_sem.at[0],
                device_id=device, device_id_type=MESH,
            )

        def send(first, last):
            def body(i, carry):
                @pl.when(i >= WINDOW)
                def _():
                    copy(i - WINDOW).wait_send()

                copy(i).start()
                return carry

            lax.fori_loop(first, last, body, 0)

        def drain():
            def body(i, carry):
                copy(i).wait_send()
                return carry

            lax.fori_loop(n - 1 - WINDOW, n - 1, body, 0)
            some = dst.at[pl.ds(0, n - 1)]
            pltpu.make_async_copy(some, some, recv_sem.at[0]).wait()

        return send, drain

    send, drain = exchange(spread, arrived, a_send, a_recv)
    gather_step(0, 0)
    send(0, 8)

    vocab = table.shape[1]
    low_count = 256
    high_count = vocab // low_count
    prompt = ids.shape[0]
    high_hot = one_hot(ids[...] // low_count == iota((prompt, high_count), 1))
    low_hot = one_hot(ids[...] % low_count == iota((prompt, low_count), 1))
    counts[...] = lax.dot_general(
        high_hot, low_hot, (((0,), (0,)), ((), ())), preferred_element_type=F32
    )

    def tally(h, total):
        piece = table[:, pl.ds(pl.multiple_of(h * low_count, low_count), low_count)]
        return total + piece.astype(F32) * counts[pl.ds(h, 1), :]

    few = table.shape[0]
    total = lax.fori_loop(0, high_count, tally, jnp.zeros((few, low_count), F32))
    pooled4 = jnp.sum(total, axis=1, keepdims=True) * (1.0 / prompt)
    pooled8 = jnp.concatenate([pooled4] * (block // few), axis=0)
    pooled8 = jnp.where(iota((block, 1), 0) // few == core, pooled8, 0.0)
    first = pooled8.astype(BF16).astype(F32)
    second = (pooled8 - first).astype(BF16).astype(F32)
    third = pooled8 - first - second
    lane = iota((block, 128), 1)
    terms = jnp.where(lane == 0, first, jnp.where(lane == 1, second, jnp.where(lane == 2, third, 0.0)))
    wgo[mx, mz // STRIDE, mz % STRIDE, :, 2 * part : 2 * part + 128] = terms.astype(BF16)

    at = 8
    total_steps = up + 3
    for step in range(1, total_steps):
        send(at, at + 8)
        at += 8
        gather_step(0, step)
    gather_step(1, 0)
    cells = TT * HH
    kt_wide = dot(kt[...], one_hot(iota((TT, cells), 1) // HH == iota((TT, cells), 0)))
    kh_wide = dot(kh[...], one_hot(iota((HH, cells), 1) % HH == iota((HH, cells), 0)))
    for s in range(TT):
        space[s * HH : (s + 1) * HH, :] = (kh_wide * kt_wide[s : s + 1, :]).astype(BF16)
    kw_wide = dot(kw[...], one_hot(iota((WW, rows), 1) // lines == iota((WW, rows), 0)))
    column_line = iota((WW, rows), 1) % lines
    for line in range(lines):
        wide[line * WW : (line + 1) * WW, :] = jnp.where(column_line == line, kw_wide, 0.0).astype(BF16)
    for step in range(1, total_steps):
        send(at, at + 8)
        at += 8
        gather_step(1, step)
    upper = pl.ds(part, part + 128)
    swap_out = pltpu.make_async_remote_copy(
        src_ref=wgo.at[:, :, :, :, upper], dst_ref=wo_other, send_sem=o_send, recv_sem=o_recv,
        device_id=other_core, device_id_type=MESH,
    )
    swap_out.start()
    send(at, n - 1)
    drain()

    quarters = rows // tile
    ycopies = []
    for r in range(quarters):
        here = slice(r * tile, (r + 1) * tile)
        full = arrived[...].reshape(rows, part)
        y_own[here, :] = dot(space[here, :], full).astype(BF16)
        ycopies.append(pltpu.make_async_remote_copy(
            src_ref=y_own.at[pl.ds(r * tile, tile)], dst_ref=y_other.at[pl.ds(r * tile, tile)],
            send_sem=y_send.at[r], recv_sem=y_recv.at[r], device_id=other_core, device_id_type=MESH,
        ))
        ycopies[-1].start()
    weight = wv.reshape(chans, part)
    own_rows = pl.ds(pl.multiple_of(core * part, part), part)
    other_rows = pl.ds(pl.multiple_of((1 - core) * part, part), part)
    for r in range(quarters):
        here = slice(r * tile, (r + 1) * tile)
        ycopies[r].wait_recv()
        value = dot(y_own[here, :], weight[own_rows, :]) + dot(y_other[here, :], weight[other_rows, :])
        filt[here, :] = (value * spec[here, :].astype(F32)).astype(BF16)
    for r in range(quarters):
        here = slice(r * tile, (r + 1) * tile)
        got = dot(space[here, :], filt[...]).astype(BF16)
        back[r * per : (r + 1) * per] = got.reshape(per, block, part)
        ycopies[r].wait_send()
    returned[me] = back[me]
    send, drain = exchange(back, returned, b_send, b_recv)
    send(0, n - 1)

    swap_out.wait()
    gathered = wgo.reshape(chans, 2 * part + 128)
    others = wo_other.reshape(chans, part + 128)
    pools = gathered[:, 2 * part : 2 * part + 128] + others[:, part : part + 128]
    chosen = one_hot(iota((chans, part), 0) == iota((chans, part), 1) + core * part)
    terms = lax.dot_general(pools, chosen, (((0,), (0,)), ((), ())), preferred_element_type=F32)
    modulation = 1.0 + jnp.sum(terms[0:8, :], axis=0, keepdims=True) + emb[...]

    def gate(r, carry):
        here = pl.ds(pl.multiple_of(r * tile, tile), tile)
        v = dot(lat[here, :], gathered[:, 0:part])
        gain[here, :] = v / (1.0 + jnp.exp(-v)) * modulation
        return carry

    lax.fori_loop(0, quarters, gate, 0)
    drain()

    half = rows // 2

    def finish(r, dst, base):
        here = pl.ds(pl.multiple_of(base + r * tile, tile), tile)
        mix = dot(wide[here, :], returned[...].reshape(rows, part)) * gain[here, :]
        dst[pl.ds(pl.multiple_of(r * tile, tile), tile), :] = mix.astype(BF16)

    mcopies = []
    for r in range(half // tile):
        finish(r, spout, (1 - core) * half)
        mcopies.append(pltpu.make_async_remote_copy(
            src_ref=spout.at[pl.ds(r * tile, tile)], dst_ref=mix_other.at[pl.ds(r * tile, tile)],
            send_sem=m_send.at[r], recv_sem=m_recv.at[r], device_id=other_core, device_id_type=MESH,
        ))
        mcopies[-1].start()
    for r in range(half // tile):
        finish(r, mix_own, core * half)
    left = pl.ds(pl.multiple_of(core * part, part), part)
    right = pl.ds(pl.multiple_of((1 - core) * part, part), part)
    for r in range(half // tile):
        here = slice(r * tile, (r + 1) * tile)
        mcopies[r].wait()
        for at, weight in ((left, gathered.at[:, part : 2 * part]), (right, others.at[:, 0:part])):
            out[here, at] = dot(mix_own[here, :], weight[own_rows, :]) + dot(
                mix_other[here, :], weight[other_rows, :]
            )


def local(nx, nz, latents, spectrum, w_value, w_gate, w_out, embed_table, prompt_ids, noise_step):
    rows, chans = latents.shape
    block, part = w_value.shape
    n = nx * nz
    core = lax.axis_index("ch")
    channel = core * part + jnp.arange(part, dtype=jnp.int32)
    emb = step_embedding(noise_step, channel, chans).reshape(1, part)
    half = rows // 2
    groups = nz // STRIDE
    hops = groups - 1
    vmem = pl.BlockSpec(memory_space=pltpu.VMEM)
    dma = pltpu.SemaphoreType.DMA
    exchanged = pltpu.VMEM((n, rows // n, part), BF16)
    plain = pltpu.VMEM((rows, part), BF16)
    summed = pl.pallas_call(
        functools.partial(kernel, nx, nz),
        out_shape=jax.ShapeDtypeStruct((half, chans), F32),
        in_specs=[vmem] * 11,
        out_specs=vmem,
        scratch_shapes=[
            exchanged, exchanged,
            pltpu.VMEM((8, 128), BF16), pltpu.VMEM((half, part), BF16),
            exchanged, exchanged,
            plain, plain, plain,
            pltpu.VMEM((rows, part), F32),
            pltpu.VMEM((nx, groups, STRIDE, block, part), BF16),
            pltpu.VMEM((nx, groups, STRIDE, block, 2 * part + 128), BF16),
            pltpu.VMEM((nx, groups, STRIDE, block, part + 128), BF16),
            pltpu.VMEM((half, part), BF16), pltpu.VMEM((half, part), BF16),
            pltpu.VMEM((embed_table.shape[1] // 256, 256), F32),
            pltpu.VMEM((rows, rows), BF16), pltpu.VMEM((rows, rows), BF16), pltpu.VMEM((rows, rows), BF16),
            dma((n,)), dma((1,)), dma((n,)), dma((1,)),
            dma((2, hops)), dma((2, hops)), dma((2, 3)), dma((2, 3)), dma((2, nx - 1)), dma((2, nx - 1)),
            dma((4,)), dma((4,)), dma, dma, dma((2,)), dma((2,)),
        ],
        compiler_params=pltpu.CompilerParams(
            collective_id=0, has_side_effects=True, vmem_limit_bytes=56 * 2**20
        ),
    )(
        latents, spectrum.reshape(rows, part), w_value, w_gate, w_out, embed_table,
        prompt_ids.reshape(-1, 1), emb, cas_table(WW), cas_table(HH), cas_table(TT),
    )
    residual = lax.dynamic_slice_in_dim(latents, core * half, half, 0)
    return (residual.astype(F32) + summed).astype(BF16)


def solution(mesh):
    nx, nz = 4, mesh.shape["sp"] // 4
    torus = Mesh(
        mesh.devices.reshape(mesh.shape["grp"], nx, nz, mesh.shape["ch"]),
        ("grp", "sp_0", "sp_1", "ch"),
    )
    in_specs = (
        P(GRP_SP, None),
        P(None, None, SP, "ch"),
        P(SP, "ch"),
        P(SP, "ch"),
        P(SP, None),
        P(SP_CH, None),
        P("grp"),
        P("grp"),
    )
    out_specs = P(GRP_SP_CH, None)
    return jax.shard_map(
        functools.partial(local, nx, nz),
        mesh=torus, in_specs=in_specs, out_specs=out_specs, check_vma=False,
    )
```

```python
import functools
import math

import jax
import jax.numpy as jnp
import numpy as np
from jax import lax
from jax.experimental import pallas as pl
from jax.experimental.pallas import tpu as pltpu
from jax.sharding import Mesh
from jax.sharding import PartitionSpec as P

TT = 16
HH = 64
WW = 128
SP_CH = ("sp_0", "sp_1", "ch")
GRP_SP = ("grp", "sp_0", "sp_1")
GRP_SP_CH = ("grp", "sp_0", "sp_1", "ch")
SP = ("sp_0", "sp_1")
F32 = jnp.float32
BF16 = jnp.bfloat16
MESH = pl.DeviceIdType.MESH
STRIDE = 4
WINDOW = 16


def cas_table(length):
    position = np.arange(length, dtype=np.int32)
    product = position[:, None] * position[None, :] % length
    phase_angle = product.astype(np.float32) * np.float32(2.0 * math.pi / length)
    table = (np.cos(phase_angle) + np.sin(phase_angle)) / np.float32(math.sqrt(length))
    return jnp.asarray(table.astype(jnp.bfloat16))


def step_embedding(noise_step, channel, channels):
    half_count = channels // 2
    lower_half = channel < half_count
    position = jnp.where(lower_half, channel, channel - half_count).astype(jnp.float32)
    frequency = jnp.exp(-math.log(10000.0) * position / half_count)
    phase_angle = noise_step[0].astype(jnp.float32) * frequency
    return jnp.where(lower_half, jnp.sin(phase_angle), jnp.cos(phase_angle))


def dot(a, b):
    return jnp.dot(a, b, preferred_element_type=F32)


def iota(shape, dim):
    return lax.broadcasted_iota(jnp.int32, shape, dim)


def one_hot(condition):
    return jnp.where(condition, 1.0, 0.0).astype(BF16)


def kernel(
    nx, nz,
    lat, spec, wv_in, wg_in, wo_in, table, ids, emb, kw, kh, kt,
    out,
    spread, arrived, spin, spout, back, returned, y_own, y_other, filt, gain,
    wv, wgo, wo_other, mix_own, mix_other, counts, space, wide, narrow,
    a_send, a_recv, b_send, b_recv, s_send, s_recv, r_send, r_recv, x_send, x_recv,
    y_send, y_recv, o_send, o_recv, m_send, m_recv,
):
    n = nx * nz
    rows, chans = lat.shape
    part = wv_in.shape[1]
    lines = rows // WW
    block = rows // n
    mx, mz, core = lax.axis_index("sp_0"), lax.axis_index("sp_1"), lax.axis_index("ch")
    me = mx * nz + mz
    other_core = {"ch": 1 - core}

    def partner(i):
        j = n - 1 - i
        zi, dx = j // nx, j % nx
        m = (zi + 1) // 2
        dz = jnp.where(zi % 2 == 1, m, nz - m) % nz
        tx, tz = (mx + dx) % nx, (mz + dz) % nz
        return {"sp_0": tx, "sp_1": tz}, tx * nz + tz

    barrier = pltpu.get_barrier_semaphore()

    def greet(i, carry):
        device, _ = partner(i)
        pl.semaphore_signal(barrier, inc=1, device_id=device, device_id_type=MESH)
        return carry

    lax.fori_loop(0, n - 1, greet, 0)
    pl.semaphore_signal(barrier, inc=1, device_id=other_core, device_id_type=MESH)

    pick = one_hot(iota((rows, WW), 0) // lines == iota((rows, WW), 1))
    spread_rows = dot(pick, kw[...]).astype(BF16)
    line_of = iota((rows, WW), 0) % lines
    for line in range(lines):
        narrow[:, line * WW : (line + 1) * WW] = jnp.where(
            line_of == line, spread_rows, jnp.zeros_like(spread_rows)
        )
    mine = pl.ds(pl.multiple_of(core * part, 128), part)
    tile = 256
    per = tile // block

    def widen(r, carry):
        at = pl.ds(pl.multiple_of(r * tile, tile), tile)
        got = dot(narrow[at, :], lat[:, mine]).astype(BF16)
        spread[pl.ds(r * per, per)] = got.reshape(per, block, part)
        return carry

    lax.fori_loop(0, rows // tile, widen, 0)
    arrived[me] = spread[me]
    wv[mx, mz // STRIDE, mz % STRIDE] = wv_in[...]
    wgo[mx, mz // STRIDE, mz % STRIDE, :, 0:part] = wg_in[...]
    wgo[mx, mz // STRIDE, mz % STRIDE, :, part : 2 * part] = wo_in[:, mine]

    pl.semaphore_wait(barrier, n)

    bufs = (wv, wgo)
    groups = nz // STRIDE
    up = (groups + 1) // 2
    down = groups - 1 - up

    def hop(stream, direction, q):
        origin = (mz // STRIDE - direction * (q - 1) + groups) % groups
        ref = bufs[stream].at[mx, origin, mz % STRIDE]
        k = (q - 1) if direction > 0 else up + q - 1
        return pltpu.make_async_remote_copy(
            src_ref=ref, dst_ref=ref,
            send_sem=s_send.at[stream, k], recv_sem=s_recv.at[stream, k],
            device_id={"sp_1": (mz + direction * STRIDE + nz) % nz}, device_id_type=MESH,
        )

    def near(stream, k):
        ref = bufs[stream].at[mx]
        step = (1, -1, 1, -1)[k]
        residue = (mz - (0, 0, 1, -1)[k] + nz) % STRIDE
        part_of = (pl.ds(0, groups), pl.ds(0, groups), pl.ds(groups // 2, groups // 2), pl.ds(0, groups // 2))[k]
        ref = ref.at[part_of, residue]
        return pltpu.make_async_remote_copy(
            src_ref=ref, dst_ref=ref,
            send_sem=r_send.at[stream, k], recv_sem=r_recv.at[stream, k],
            device_id={"sp_1": (mz + step + nz) % nz}, device_id_type=MESH,
        )

    def across(stream, k):
        step = (1, -1, 1, -1)[k]
        column = (mx - (0, 0, 1, -1)[k] + nx) % nx
        part_of = (pl.ds(0, groups), pl.ds(0, groups), pl.ds(groups // 2, groups // 2), pl.ds(0, groups // 2))[k]
        ref = bufs[stream].at[column, part_of]
        return pltpu.make_async_remote_copy(
            src_ref=ref, dst_ref=ref,
            send_sem=x_send.at[stream, k], recv_sem=x_recv.at[stream, k],
            device_id={"sp_0": (mx + step + nx) % nx}, device_id_type=MESH,
        )

    def gather_step(stream, step):
        if 0 < step <= up:
            hop(stream, 1, step).wait_recv()
        if 0 < step <= down:
            hop(stream, -1, step).wait_recv()
        if step < up:
            hop(stream, 1, step + 1).start()
        if step < down:
            hop(stream, -1, step + 1).start()
        for first, copies in ((up, near), (up + 2, across)):
            if step == first:
                copies(stream, 0).start()
                copies(stream, 1).start()
            if step == first + 1:
                copies(stream, 0).wait_recv()
                copies(stream, 1).wait_recv()
                copies(stream, 2).start()
                copies(stream, 3).start()
            if step == first + 2:
                copies(stream, 2).wait_recv()
                copies(stream, 3).wait_recv()
        if step == up + 4:
            for q in range(up):
                hop(stream, 1, q + 1).wait_send()
            for q in range(down):
                hop(stream, -1, q + 1).wait_send()
            for copies in (near, across):
                for k in range(4):
                    copies(stream, k).wait_send()

    def exchange(src, dst, send_sem, recv_sem):
        def copy(i):
            device, target = partner(i)
            return pltpu.make_async_remote_copy(
                src_ref=src.at[target], dst_ref=dst.at[me],
                send_sem=send_sem.at[i], recv_sem=recv_sem.at[0],
                device_id=device, device_id_type=MESH,
            )

        def send(first, last):
            def body(i, carry):
                @pl.when(i >= WINDOW)
                def _():
                    copy(i - WINDOW).wait_send()

                copy(i).start()
                return carry

            lax.fori_loop(first, last, body, 0)

        def drain():
            def body(i, carry):
                copy(i).wait_send()
                return carry

            lax.fori_loop(n - 1 - WINDOW, n - 1, body, 0)
            some = dst.at[pl.ds(0, n - 1)]
            pltpu.make_async_copy(some, some, recv_sem.at[0]).wait()

        return send, drain

    send, drain = exchange(spread, arrived, a_send, a_recv)
    gather_step(0, 0)
    send(0, 8)

    vocab = table.shape[1]
    low_count = 256
    high_count = vocab // low_count
    prompt = ids.shape[1]
    high_hot = one_hot(ids[...] // low_count == iota((high_count, prompt), 0))
    low_hot = one_hot(ids[...] % low_count == iota((low_count, prompt), 0))
    counts[...] = lax.dot_general(
        high_hot, low_hot, (((1,), (1,)), ((), ())), preferred_element_type=F32
    )

    def tally(h, total):
        piece = table[:, pl.ds(pl.multiple_of(h * low_count, low_count), low_count)]
        return total + piece.astype(F32) * counts[pl.ds(h, 1), :]

    few = table.shape[0]
    total = lax.fori_loop(0, high_count, tally, jnp.zeros((few, low_count), F32))
    pooled4 = jnp.sum(total, axis=1, keepdims=True) * (1.0 / prompt)
    pooled8 = jnp.concatenate([pooled4] * (block // few), axis=0)
    pooled8 = jnp.where(iota((block, 1), 0) // few == core, pooled8, 0.0)
    first = pooled8.astype(BF16).astype(F32)
    second = (pooled8 - first).astype(BF16).astype(F32)
    third = pooled8 - first - second
    lane = iota((block, 128), 1)
    terms = jnp.where(lane == 0, first, jnp.where(lane == 1, second, jnp.where(lane == 2, third, 0.0)))
    wgo[mx, mz // STRIDE, mz % STRIDE, :, 2 * part : 2 * part + 128] = terms.astype(BF16)

    total_steps = up + 4

    def send_beside(stream, first, last):
        pace = (last - first) // total_steps
        at = first
        for step in range(1, total_steps + 1):
            send(at, at + pace)
            at += pace
            gather_step(stream, step)
        send(at, last)

    cells = TT * HH
    kt_wide = dot(kt[...], one_hot(iota((TT, cells), 1) // HH == iota((TT, cells), 0)))
    kh_wide = dot(kh[...], one_hot(iota((HH, cells), 1) % HH == iota((HH, cells), 0)))
    for s in range(TT):
        space[s * HH : (s + 1) * HH, :] = (kh_wide * kt_wide[s : s + 1, :]).astype(BF16)
    kw_wide = dot(kw[...], one_hot(iota((WW, rows), 1) // lines == iota((WW, rows), 0)))
    column_line = iota((WW, rows), 1) % lines
    for line in range(lines):
        wide[line * WW : (line + 1) * WW, :] = jnp.where(column_line == line, kw_wide, 0.0).astype(BF16)
    send_beside(0, 8, n - 1)
    drain()

    quarters = rows // tile
    ycopies = []
    for r in range(quarters):
        here = slice(r * tile, (r + 1) * tile)
        full = arrived[...].reshape(rows, part)
        y_own[here, :] = dot(space[here, :], full).astype(BF16)
        ycopies.append(pltpu.make_async_remote_copy(
            src_ref=y_own.at[pl.ds(r * tile, tile)], dst_ref=y_other.at[pl.ds(r * tile, tile)],
            send_sem=y_send.at[r], recv_sem=y_recv.at[r], device_id=other_core, device_id_type=MESH,
        ))
        ycopies[-1].start()
    weight = wv.reshape(chans, part)
    own_rows = pl.ds(pl.multiple_of(core * part, part), part)
    other_rows = pl.ds(pl.multiple_of((1 - core) * part, part), part)
    for r in range(quarters):
        here = slice(r * tile, (r + 1) * tile)
        ycopies[r].wait_recv()
        value = dot(y_own[here, :], weight[own_rows, :]) + dot(y_other[here, :], weight[other_rows, :])
        filt[here, :] = (value * spec[here, :].astype(F32)).astype(BF16)
    for r in range(quarters):
        here = slice(r * tile, (r + 1) * tile)
        got = dot(space[here, :], filt[...]).astype(BF16)
        back[r * per : (r + 1) * per] = got.reshape(per, block, part)
        ycopies[r].wait_send()
    returned[me] = back[me]
    send, drain = exchange(back, returned, b_send, b_recv)
    gather_step(1, 0)
    send_beside(1, 0, n - 1)

    upper = pl.ds(part, part + 128)
    swap_out = pltpu.make_async_remote_copy(
        src_ref=wgo.at[:, :, :, :, upper], dst_ref=wo_other, send_sem=o_send, recv_sem=o_recv,
        device_id=other_core, device_id_type=MESH,
    )
    swap_out.start()
    swap_out.wait()
    gathered = wgo.reshape(chans, 2 * part + 128)
    others = wo_other.reshape(chans, part + 128)
    pools = gathered[:, 2 * part : 2 * part + 128] + others[:, part : part + 128]
    chosen = one_hot(iota((chans, part), 0) == iota((chans, part), 1) + core * part)
    terms = lax.dot_general(pools, chosen, (((0,), (0,)), ((), ())), preferred_element_type=F32)
    modulation = 1.0 + jnp.sum(terms[0:8, :], axis=0, keepdims=True) + emb[...]

    def gate(r, carry):
        here = pl.ds(pl.multiple_of(r * tile, tile), tile)
        v = dot(lat[here, :], gathered[:, 0:part])
        gain[here, :] = v / (1.0 + jnp.exp(-v)) * modulation
        return carry

    lax.fori_loop(0, quarters, gate, 0)
    drain()

    half = rows // 2

    def finish(r, dst, base):
        here = pl.ds(pl.multiple_of(base + r * tile, tile), tile)
        mix = dot(wide[here, :], returned[...].reshape(rows, part)) * gain[here, :]
        dst[pl.ds(pl.multiple_of(r * tile, tile), tile), :] = mix.astype(BF16)

    mcopies = []
    for r in range(half // tile):
        finish(r, spout, (1 - core) * half)
        mcopies.append(pltpu.make_async_remote_copy(
            src_ref=spout.at[pl.ds(r * tile, tile)], dst_ref=mix_other.at[pl.ds(r * tile, tile)],
            send_sem=m_send.at[r], recv_sem=m_recv.at[r], device_id=other_core, device_id_type=MESH,
        ))
        mcopies[-1].start()
    for r in range(half // tile):
        finish(r, mix_own, core * half)
    left = pl.ds(pl.multiple_of(core * part, part), part)
    right = pl.ds(pl.multiple_of((1 - core) * part, part), part)
    for r in range(half // tile):
        here = slice(r * tile, (r + 1) * tile)
        mcopies[r].wait()
        for at, weight in ((left, gathered.at[:, part : 2 * part]), (right, others.at[:, 0:part])):
            out[here, at] = dot(mix_own[here, :], weight[own_rows, :]) + dot(
                mix_other[here, :], weight[other_rows, :]
            )


def local(nx, nz, latents, spectrum, w_value, w_gate, w_out, embed_table, prompt_ids, noise_step):
    rows, chans = latents.shape
    block, part = w_value.shape
    n = nx * nz
    core = lax.axis_index("ch")
    channel = core * part + jnp.arange(part, dtype=jnp.int32)
    emb = step_embedding(noise_step, channel, chans).reshape(1, part)
    half = rows // 2
    groups = nz // STRIDE
    hops = groups - 1
    vmem = pl.BlockSpec(memory_space=pltpu.VMEM)
    dma = pltpu.SemaphoreType.DMA
    exchanged = pltpu.VMEM((n, rows // n, part), BF16)
    plain = pltpu.VMEM((rows, part), BF16)
    summed = pl.pallas_call(
        functools.partial(kernel, nx, nz),
        out_shape=jax.ShapeDtypeStruct((half, chans), F32),
        in_specs=[vmem] * 11,
        out_specs=vmem,
        scratch_shapes=[
            exchanged, exchanged,
            pltpu.VMEM((8, 128), BF16), pltpu.VMEM((half, part), BF16),
            exchanged, exchanged,
            plain, plain, plain,
            pltpu.VMEM((rows, part), F32),
            pltpu.VMEM((nx, groups, STRIDE, block, part), BF16),
            pltpu.VMEM((nx, groups, STRIDE, block, 2 * part + 128), BF16),
            pltpu.VMEM((nx, groups, STRIDE, block, part + 128), BF16),
            pltpu.VMEM((half, part), BF16), pltpu.VMEM((half, part), BF16),
            pltpu.VMEM((embed_table.shape[1] // 256, 256), F32),
            pltpu.VMEM((rows, rows), BF16), pltpu.VMEM((rows, rows), BF16), pltpu.VMEM((rows, rows), BF16),
            dma((n,)), dma((1,)), dma((n,)), dma((1,)),
            dma((2, hops)), dma((2, hops)), dma((2, 4)), dma((2, 4)), dma((2, 4)), dma((2, 4)),
            dma((4,)), dma((4,)), dma, dma, dma((2,)), dma((2,)),
        ],
        compiler_params=pltpu.CompilerParams(
            collective_id=0, has_side_effects=True, vmem_limit_bytes=56 * 2**20
        ),
    )(
        latents, spectrum.reshape(rows, part), w_value, w_gate, w_out, embed_table,
        prompt_ids.reshape(1, -1), emb, cas_table(WW), cas_table(HH), cas_table(TT),
    )
    residual = lax.dynamic_slice_in_dim(latents, core * half, half, 0)
    return (residual.astype(F32) + summed).astype(BF16)


def solution(mesh):
    nx, nz = 4, mesh.shape["sp"] // 4
    torus = Mesh(
        mesh.devices.reshape(mesh.shape["grp"], nx, nz, mesh.shape["ch"]),
        ("grp", "sp_0", "sp_1", "ch"),
    )
    in_specs = (
        P(GRP_SP, None),
        P(None, None, SP, "ch"),
        P(SP, "ch"),
        P(SP, "ch"),
        P(SP, None),
        P(SP_CH, None),
        P("grp"),
        P("grp"),
    )
    out_specs = P(GRP_SP_CH, None)
    return jax.shard_map(
        functools.partial(local, nx, nz),
        mesh=torus, in_specs=in_specs, out_specs=out_specs, check_vma=False,
    )
```

```python
import functools
import math

import jax
import jax.numpy as jnp
import numpy as np
from jax import lax
from jax.experimental import pallas as pl
from jax.experimental.pallas import tpu as pltpu
from jax.sharding import Mesh
from jax.sharding import PartitionSpec as P

TT = 16
HH = 64
WW = 128
SP_CH = ("sp_0", "sp_1", "ch")
GRP_SP = ("grp", "sp_0", "sp_1")
GRP_SP_CH = ("grp", "sp_0", "sp_1", "ch")
SP = ("sp_0", "sp_1")
F32 = jnp.float32
BF16 = jnp.bfloat16
MESH = pl.DeviceIdType.MESH
STRIDE = 4
WINDOW = 16


def cas_table(length):
    position = np.arange(length, dtype=np.int32)
    product = position[:, None] * position[None, :] % length
    phase_angle = product.astype(np.float32) * np.float32(2.0 * math.pi / length)
    table = (np.cos(phase_angle) + np.sin(phase_angle)) / np.float32(math.sqrt(length))
    return jnp.asarray(table.astype(jnp.bfloat16))


def step_embedding(noise_step, channel, channels):
    half_count = channels // 2
    lower_half = channel < half_count
    position = jnp.where(lower_half, channel, channel - half_count).astype(jnp.float32)
    frequency = jnp.exp(-math.log(10000.0) * position / half_count)
    phase_angle = noise_step[0].astype(jnp.float32) * frequency
    return jnp.where(lower_half, jnp.sin(phase_angle), jnp.cos(phase_angle))


def dot(a, b):
    return jnp.dot(a, b, preferred_element_type=F32)


def iota(shape, dim):
    return lax.broadcasted_iota(jnp.int32, shape, dim)


def one_hot(condition):
    return jnp.where(condition, 1.0, 0.0).astype(BF16)


def kernel(
    nx, nz,
    lat, spec, wv_in, wg_in, wo_in, table, ids, emb, kw, kh, kt,
    out,
    spread, arrived, spin, spout, back, returned, y_own, y_other, filt, gain,
    wall, wo_other, mix_own, mix_other, counts, space, wide, narrow,
    hello, a_send, a_recv, b_send, b_recv, s_send, s_recv, r_send, r_recv,
    y_send, y_recv, o_send, o_recv, m_send, m_recv,
):
    n = nx * nz
    rows, chans = lat.shape
    part = wv_in.shape[1]
    lines = rows // WW
    block = rows // n
    mx, mz, core = lax.axis_index("sp_0"), lax.axis_index("sp_1"), lax.axis_index("ch")
    me = mx * nz + mz
    other_core = {"ch": 1 - core}

    def partner(i):
        j = n - 1 - i
        zi, dx = j // nx, j % nx
        m = (zi + 1) // 2
        dz = jnp.where(zi % 2 == 1, m, nz - m) % nz
        tx, tz = (mx + dx) % nx, (mz + dz) % nz
        return {"sp_0": tx, "sp_1": tz}, tx * nz + tz

    def layered(i):
        tx, tz = (mx + i % nx) % nx, i // nx
        return {"sp_0": tx, "sp_1": tz}, tx * nz + tz

    barrier = pltpu.get_barrier_semaphore()
    for dx in range(1, nx):
        pl.semaphore_signal(
            barrier, inc=1, device_id={"sp_0": (mx + dx) % nx}, device_id_type=MESH
        )
    pl.semaphore_signal(barrier, inc=1, device_id=other_core, device_id_type=MESH)
    pl.semaphore_wait(barrier, jnp.where(mz > 0, 2 * nx, nx))

    def tell(dx, carry):
        device = {"sp_0": (mx + dx) % nx, "sp_1": mz + 1}
        pl.semaphore_signal(barrier, inc=1, device_id=device, device_id_type=MESH)
        return carry

    lax.fori_loop(0, jnp.where(mz < nz - 1, nx, 0), tell, 0)

    def greet(i, carry):
        device, _ = layered(i)
        pl.semaphore_signal(hello.at[mz], inc=1, device_id=device, device_id_type=MESH)
        return carry

    lax.fori_loop(0, nx * mz, greet, 0)

    def hear(layer):
        @pl.when(layer > mz)
        def _():
            pl.semaphore_wait(hello.at[layer], nx)

    pick = one_hot(iota((rows, WW), 0) // lines == iota((rows, WW), 1))
    spread_rows = dot(pick, kw[...]).astype(BF16)
    line_of = iota((rows, WW), 0) % lines
    for line in range(lines):
        narrow[:, line * WW : (line + 1) * WW] = jnp.where(
            line_of == line, spread_rows, jnp.zeros_like(spread_rows)
        )
    mine = pl.ds(pl.multiple_of(core * part, 128), part)
    tile = 256
    per = tile // block

    def widen(r, carry):
        at = pl.ds(pl.multiple_of(r * tile, tile), tile)
        got = dot(narrow[at, :], lat[:, mine]).astype(BF16)
        spread[pl.ds(r * per, per)] = got.reshape(per, block, part)
        return carry

    lax.fori_loop(0, rows // tile, widen, 0)
    arrived[me] = spread[me]
    wall[mx, mz // STRIDE, mz % STRIDE, :, 0:part] = wv_in[...]
    wall[mx, mz // STRIDE, mz % STRIDE, :, part : 2 * part] = wg_in[...]
    wall[mx, mz // STRIDE, mz % STRIDE, :, 2 * part : 3 * part] = wo_in[:, mine]

    groups = nz // STRIDE
    up = (groups + 1) // 2
    down = groups - 1 - up

    first_part = pl.ds(0, part)
    later_part = pl.ds(part, 2 * part + 128)

    def hop(direction, q):
        origin = (mz // STRIDE - direction * (q - 1) + groups) % groups
        ref = wall.at[mx, origin, mz % STRIDE]
        k = (q - 1) if direction > 0 else up + q - 1
        return pltpu.make_async_remote_copy(
            src_ref=ref, dst_ref=ref, send_sem=s_send.at[k], recv_sem=s_recv.at[k],
            device_id={"sp_1": (mz + direction * STRIDE + nz) % nz}, device_id_type=MESH,
        )

    def hop_in(q):
        hop(1, q).wait_recv()
        if q <= down:
            hop(-1, q).wait_recv()

    def hop_out(q):
        hop(1, q).start()
        if q <= down:
            hop(-1, q).start()

    def group_span(k):
        return ((0, groups), (0, groups), (groups // 2, groups), (0, groups // 2))[k]

    def piece(stage, k, g, count):
        step = (1, -1, 1, -1)[k]
        back_by = (0, 0, 1, -1)[k]
        if stage:
            lanes = (first_part, later_part)[stage - 1]
            ref = wall.at[(mx - back_by + nx) % nx, pl.ds(g, count), :, :, lanes]
            device = {"sp_0": (mx + step + nx) % nx}
        else:
            ref = wall.at[mx, pl.ds(g, count), (mz - back_by + nz) % STRIDE]
            device = {"sp_1": (mz + step + nz) % nz}
        return pltpu.make_async_remote_copy(
            src_ref=ref, dst_ref=ref, send_sem=r_send.at[stage, k], recv_sem=r_recv.at[stage, k],
            device_id=device, device_id_type=MESH,
        )

    def whole(stage, k):
        low, high = group_span(k)
        return piece(stage, k, low, high - low)

    def exchange(src, dst, send_sem, recv_sem, layers):
        count = n if layers else n - 1

        def copy(i):
            device, target = layered(i) if layers else partner(i)
            return pltpu.make_async_remote_copy(
                src_ref=src.at[target], dst_ref=dst.at[me],
                send_sem=send_sem.at[i], recv_sem=recv_sem.at[0],
                device_id=device, device_id_type=MESH,
            )

        def there(i, do):
            if layers:
                pl.when(i != mz * nx)(do)
            else:
                do()

        def send(first, last, listen=False):
            def body(i, carry):
                @pl.when(i >= WINDOW)
                def _():
                    there(i - WINDOW, lambda: copy(i - WINDOW).wait_send())

                if listen:
                    pl.when(i % nx == 0)(lambda: hear(i // nx))
                there(i, lambda: copy(i).start())
                return carry

            lax.fori_loop(first, last, body, 0)

        def drain():
            def body(i, carry):
                there(i, lambda: copy(i).wait_send())
                return carry

            lax.fori_loop(count - WINDOW, count, body, 0)
            some = dst.at[pl.ds(0, n - 1)]
            pltpu.make_async_copy(some, some, recv_sem.at[0]).wait()

        return send, drain

    send, drain = exchange(spread, arrived, a_send, a_recv, True)

    vocab = table.shape[1]
    low_count = 256
    high_count = vocab // low_count
    prompt = ids.shape[1]
    high_hot = one_hot(ids[...] // low_count == iota((high_count, prompt), 0))
    low_hot = one_hot(ids[...] % low_count == iota((low_count, prompt), 0))
    counts[...] = lax.dot_general(
        high_hot, low_hot, (((1,), (1,)), ((), ())), preferred_element_type=F32
    )

    def tally(h, total):
        piece = table[:, pl.ds(pl.multiple_of(h * low_count, low_count), low_count)]
        return total + piece.astype(F32) * counts[pl.ds(h, 1), :]

    few = table.shape[0]
    total = lax.fori_loop(0, high_count, tally, jnp.zeros((few, low_count), F32))
    pooled4 = jnp.sum(total, axis=1, keepdims=True) * (1.0 / prompt)
    pooled8 = jnp.concatenate([pooled4] * (block // few), axis=0)
    pooled8 = jnp.where(iota((block, 1), 0) // few == core, pooled8, 0.0)
    first = pooled8.astype(BF16).astype(F32)
    second = (pooled8 - first).astype(BF16).astype(F32)
    third = pooled8 - first - second
    lane = iota((block, 128), 1)
    terms = jnp.where(lane == 0, first, jnp.where(lane == 1, second, jnp.where(lane == 2, third, 0.0)))
    wall[mx, mz // STRIDE, mz % STRIDE, :, 3 * part : 3 * part + 128] = terms.astype(BF16)

    heard = nz - 4 - (mz * (nz - 5)) // nz
    send(0, heard * nx, True)

    def hear_rest(layer, carry):
        hear(layer)
        return carry

    lax.fori_loop(heard, nz, hear_rest, 0)
    hop_out(1)

    def send_pieces(stage, at, each, slack):
        for pair in ((0, 1), (2, 3)):
            count = group_span(pair[0])[1] - group_span(pair[0])[0]

            def body(g, carry, at=at, pair=pair):
                for k in pair:
                    piece(stage, k, group_span(k)[0] + g, 1).start()
                send(at + g * each, at + (g + 1) * each)
                return carry

            lax.fori_loop(0, count, body, 0)
            at += count * each
            send(at, at + slack)
            at += slack
            for k in pair:
                whole(stage, k).wait_recv()
        return at

    cells = TT * HH
    kt_wide = dot(kt[...], one_hot(iota((TT, cells), 1) // HH == iota((TT, cells), 0)))
    kh_wide = dot(kh[...], one_hot(iota((HH, cells), 1) % HH == iota((HH, cells), 0)))
    for s in range(TT):
        space[s * HH : (s + 1) * HH, :] = (kh_wide * kt_wide[s : s + 1, :]).astype(BF16)
    kw_wide = dot(kw[...], one_hot(iota((WW, rows), 1) // lines == iota((WW, rows), 0)))
    column_line = iota((WW, rows), 1) % lines
    for line in range(lines):
        wide[line * WW : (line + 1) * WW, :] = jnp.where(column_line == line, kw_wide, 0.0).astype(BF16)
    begin = heard * nx
    left_over = n - begin

    def until(share):
        return begin + left_over * share // 128

    done = begin
    for q in range(1, up + 1):
        send(done, until(11 * q))
        done = until(11 * q)
        hop_in(q)
        if q < up:
            hop_out(q + 1)
    share = 11 * up
    for stage in (0, 1):
        for pair in ((0, 1), (2, 3)):
            count = group_span(pair[0])[1] - group_span(pair[0])[0]
            for g in range(count):
                for k in pair:
                    piece(stage, k, group_span(k)[0] + g, 1).start()
                share += 1
                send(done, until(share))
                done = until(share)
            share += 7
            send(done, until(share))
            done = until(share)
            for k in pair:
                whole(stage, k).wait_recv()
    send(done, n)
    drain()

    quarters = rows // tile
    ycopies = []
    for r in range(quarters):
        here = slice(r * tile, (r + 1) * tile)
        full = arrived[...].reshape(rows, part)
        y_own[here, :] = dot(space[here, :], full).astype(BF16)
        ycopies.append(pltpu.make_async_remote_copy(
            src_ref=y_own.at[pl.ds(r * tile, tile)], dst_ref=y_other.at[pl.ds(r * tile, tile)],
            send_sem=y_send.at[r], recv_sem=y_recv.at[r], device_id=other_core, device_id_type=MESH,
        ))
        ycopies[-1].start()
    gathered = wall.reshape(chans, 3 * part + 128)
    weight = gathered.at[:, 0:part]
    own_rows = pl.ds(pl.multiple_of(core * part, part), part)
    other_rows = pl.ds(pl.multiple_of((1 - core) * part, part), part)
    for r in range(quarters):
        here = slice(r * tile, (r + 1) * tile)
        ycopies[r].wait_recv()
        value = dot(y_own[here, :], weight[own_rows, :]) + dot(y_other[here, :], weight[other_rows, :])
        filt[here, :] = (value * spec[here, :].astype(F32)).astype(BF16)
    for r in range(quarters):
        here = slice(r * tile, (r + 1) * tile)
        got = dot(space[here, :], filt[...]).astype(BF16)
        back[r * per : (r + 1) * per] = got.reshape(per, block, part)
        ycopies[r].wait_send()
    returned[me] = back[me]
    send, drain = exchange(back, returned, b_send, b_recv, False)
    at = send_pieces(2, 0, 6, 16)
    send(at, n - 1)
    for q in range(1, up + 1):
        hop(1, q).wait_send()
        if q <= down:
            hop(-1, q).wait_send()
    for stage in range(3):
        for k in range(4):
            whole(stage, k).wait_send()

    upper = pl.ds(2 * part, part + 128)
    swap_out = pltpu.make_async_remote_copy(
        src_ref=wall.at[:, :, :, :, upper], dst_ref=wo_other, send_sem=o_send, recv_sem=o_recv,
        device_id=other_core, device_id_type=MESH,
    )
    swap_out.start()
    swap_out.wait()
    others = wo_other.reshape(chans, part + 128)
    pools = gathered[:, 3 * part : 3 * part + 128] + others[:, part : part + 128]
    chosen = one_hot(iota((chans, part), 0) == iota((chans, part), 1) + core * part)
    terms = lax.dot_general(pools, chosen, (((0,), (0,)), ((), ())), preferred_element_type=F32)
    modulation = 1.0 + jnp.sum(terms[0:8, :], axis=0, keepdims=True) + emb[...]

    def gate(r, carry):
        here = pl.ds(pl.multiple_of(r * tile, tile), tile)
        v = dot(lat[here, :], gathered[:, part : 2 * part])
        gain[here, :] = v / (1.0 + jnp.exp(-v)) * modulation
        return carry

    lax.fori_loop(0, quarters, gate, 0)
    drain()

    half = rows // 2

    def finish(r, dst, base):
        here = pl.ds(pl.multiple_of(base + r * tile, tile), tile)
        mix = dot(wide[here, :], returned[...].reshape(rows, part)) * gain[here, :]
        dst[pl.ds(pl.multiple_of(r * tile, tile), tile), :] = mix.astype(BF16)

    mcopies = []
    for r in range(half // tile):
        finish(r, spout, (1 - core) * half)
        mcopies.append(pltpu.make_async_remote_copy(
            src_ref=spout.at[pl.ds(r * tile, tile)], dst_ref=mix_other.at[pl.ds(r * tile, tile)],
            send_sem=m_send.at[r], recv_sem=m_recv.at[r], device_id=other_core, device_id_type=MESH,
        ))
        mcopies[-1].start()
    for r in range(half // tile):
        finish(r, mix_own, core * half)
    left = pl.ds(pl.multiple_of(core * part, part), part)
    right = pl.ds(pl.multiple_of((1 - core) * part, part), part)
    for r in range(half // tile):
        here = slice(r * tile, (r + 1) * tile)
        mcopies[r].wait()
        for at, weight in ((left, gathered.at[:, 2 * part : 3 * part]), (right, others.at[:, 0:part])):
            out[here, at] = dot(mix_own[here, :], weight[own_rows, :]) + dot(
                mix_other[here, :], weight[other_rows, :]
            )


def local(nx, nz, latents, spectrum, w_value, w_gate, w_out, embed_table, prompt_ids, noise_step):
    rows, chans = latents.shape
    block, part = w_value.shape
    n = nx * nz
    core = lax.axis_index("ch")
    channel = core * part + jnp.arange(part, dtype=jnp.int32)
    emb = step_embedding(noise_step, channel, chans).reshape(1, part)
    half = rows // 2
    groups = nz // STRIDE
    hops = groups - 1
    vmem = pl.BlockSpec(memory_space=pltpu.VMEM)
    dma = pltpu.SemaphoreType.DMA
    exchanged = pltpu.VMEM((n, rows // n, part), BF16)
    plain = pltpu.VMEM((rows, part), BF16)
    summed = pl.pallas_call(
        functools.partial(kernel, nx, nz),
        out_shape=jax.ShapeDtypeStruct((half, chans), F32),
        in_specs=[vmem] * 11,
        out_specs=vmem,
        scratch_shapes=[
            exchanged, exchanged,
            pltpu.VMEM((8, 128), BF16), pltpu.VMEM((half, part), BF16),
            exchanged, exchanged,
            plain, plain, plain,
            pltpu.VMEM((rows, part), F32),
            pltpu.VMEM((nx, groups, STRIDE, block, 3 * part + 128), BF16),
            pltpu.VMEM((nx, groups, STRIDE, block, part + 128), BF16),
            pltpu.VMEM((half, part), BF16), pltpu.VMEM((half, part), BF16),
            pltpu.VMEM((embed_table.shape[1] // 256, 256), F32),
            pltpu.VMEM((rows, rows), BF16), pltpu.VMEM((rows, rows), BF16), pltpu.VMEM((rows, rows), BF16),
            pltpu.SemaphoreType.REGULAR((nz,)), dma((n,)), dma((1,)), dma((n,)), dma((1,)),
            dma((hops,)), dma((hops,)), dma((3, 4)), dma((3, 4)),
            dma((4,)), dma((4,)), dma, dma, dma((2,)), dma((2,)),
        ],
        compiler_params=pltpu.CompilerParams(
            collective_id=0, has_side_effects=True, vmem_limit_bytes=56 * 2**20
        ),
    )(
        latents, spectrum.reshape(rows, part), w_value, w_gate, w_out, embed_table,
        prompt_ids.reshape(1, -1), emb, cas_table(WW), cas_table(HH), cas_table(TT),
    )
    residual = lax.dynamic_slice_in_dim(latents, core * half, half, 0)
    return (residual.astype(F32) + summed).astype(BF16)


def solution(mesh):
    nx, nz = 4, mesh.shape["sp"] // 4
    torus = Mesh(
        mesh.devices.reshape(mesh.shape["grp"], nx, nz, mesh.shape["ch"]),
        ("grp", "sp_0", "sp_1", "ch"),
    )
    in_specs = (
        P(GRP_SP, None),
        P(None, None, SP, "ch"),
        P(SP, "ch"),
        P(SP, "ch"),
        P(SP, None),
        P(SP_CH, None),
        P("grp"),
        P("grp"),
    )
    out_specs = P(GRP_SP_CH, None)
    return jax.shard_map(
        functools.partial(local, nx, nz),
        mesh=torus, in_specs=in_specs, out_specs=out_specs, check_vma=False,
    )
```

```python
import functools
import math

import jax
import jax.numpy as jnp
import numpy as np
from jax import lax
from jax.experimental import pallas as pl
from jax.experimental.pallas import tpu as pltpu
from jax.sharding import Mesh
from jax.sharding import PartitionSpec as P

TT = 16
HH = 64
WW = 128
SP_CH = ("sp_0", "sp_1", "ch")
GRP_SP = ("grp", "sp_0", "sp_1")
GRP_SP_CH = ("grp", "sp_0", "sp_1", "ch")
SP = ("sp_0", "sp_1")
F32 = jnp.float32
BF16 = jnp.bfloat16
MESH = pl.DeviceIdType.MESH
STRIDE = 4
WINDOW = 16


def cas_table(length):
    position = np.arange(length, dtype=np.int32)
    product = position[:, None] * position[None, :] % length
    phase_angle = product.astype(np.float32) * np.float32(2.0 * math.pi / length)
    table = (np.cos(phase_angle) + np.sin(phase_angle)) / np.float32(math.sqrt(length))
    return jnp.asarray(table.astype(jnp.bfloat16))


def step_embedding(noise_step, channel, channels):
    half_count = channels // 2
    lower_half = channel < half_count
    position = jnp.where(lower_half, channel, channel - half_count).astype(jnp.float32)
    frequency = jnp.exp(-math.log(10000.0) * position / half_count)
    phase_angle = noise_step[0].astype(jnp.float32) * frequency
    return jnp.where(lower_half, jnp.sin(phase_angle), jnp.cos(phase_angle))


def dot(a, b):
    return jnp.dot(a, b, preferred_element_type=F32)


def iota(shape, dim):
    return lax.broadcasted_iota(jnp.int32, shape, dim)


def one_hot(condition):
    return jnp.where(condition, 1.0, 0.0).astype(BF16)


def kernel(
    nx, nz,
    lat, spec, wv_in, wg_in, wo_in, table, ids, emb, kw, kh, kt,
    out,
    spread, arrived, spin, spout, back, returned, y_own, y_other, filt, gain,
    wall, wo_other, mix_own, mix_other, counts, space, wide, narrow,
    hello, ring_hello, a_send, a_recv, b_send, b_recv, s_send, s_recv, r_send, r_recv,
    y_send, y_recv, o_send, o_recv, m_send, m_recv,
):
    n = nx * nz
    rows, chans = lat.shape
    part = wv_in.shape[1]
    lines = rows // WW
    block = rows // n
    mx, mz, core = lax.axis_index("sp_0"), lax.axis_index("sp_1"), lax.axis_index("ch")
    me = mx * nz + mz
    other_core = {"ch": 1 - core}

    def partner(i):
        j = n - 1 - i
        zi, dx = j // nx, j % nx
        m = (zi + 1) // 2
        dz = jnp.where(zi % 2 == 1, m, nz - m) % nz
        tx, tz = (mx + dx) % nx, (mz + dz) % nz
        return {"sp_0": tx, "sp_1": tz}, tx * nz + tz

    def below(i):
        return {"sp_0": (mx + i % nx) % nx, "sp_1": i // nx}

    barrier = pltpu.get_barrier_semaphore()
    for dx in range(1, nx):
        pl.semaphore_signal(
            barrier, inc=1, device_id={"sp_0": (mx + dx) % nx}, device_id_type=MESH
        )
    pl.semaphore_signal(barrier, inc=1, device_id=other_core, device_id_type=MESH)
    pl.semaphore_wait(barrier, jnp.where(mz > 0, 2 * nx, nx))

    def tell(dx, carry):
        device = {"sp_0": (mx + dx) % nx, "sp_1": mz + 1}
        pl.semaphore_signal(barrier, inc=1, device_id=device, device_id_type=MESH)
        return carry

    lax.fori_loop(0, jnp.where(mz < nz - 1, nx, 0), tell, 0)

    def greet(i, carry):
        pl.semaphore_signal(hello.at[mz], inc=1, device_id=below(i), device_id_type=MESH)
        return carry

    lax.fori_loop(0, nx * mz, greet, 0)

    def hear(layer):
        @pl.when(layer > mz)
        def _():
            pl.semaphore_wait(hello.at[layer], nx)

    ring_steps = (1, -1, STRIDE, -STRIDE)
    above = 0
    for step in ring_steps:
        layer = (mz + step + nz) % nz

        @pl.when(layer < mz)
        def _():
            pl.semaphore_signal(ring_hello, inc=1, device_id={"sp_1": layer}, device_id_type=MESH)

        above = above + jnp.where(layer > mz, 1, 0)

    pick = one_hot(iota((rows, WW), 0) // lines == iota((rows, WW), 1))
    spread_rows = dot(pick, kw[...]).astype(BF16)
    line_of = iota((rows, WW), 0) % lines
    for line in range(lines):
        narrow[:, line * WW : (line + 1) * WW] = jnp.where(
            line_of == line, spread_rows, jnp.zeros_like(spread_rows)
        )
    mine = pl.ds(pl.multiple_of(core * part, 128), part)
    tile = 256
    per = tile // block

    def widen(r, carry):
        at = pl.ds(pl.multiple_of(r * tile, tile), tile)
        got = dot(narrow[at, :], lat[:, mine]).astype(BF16)
        spread[pl.ds(r * per, per)] = got.reshape(per, block, part)
        return carry

    lax.fori_loop(0, rows // tile, widen, 0)
    arrived[me] = spread[me]
    wall[mx, mz // STRIDE, mz % STRIDE, :, 0:part] = wv_in[...]
    wall[mx, mz // STRIDE, mz % STRIDE, :, part : 2 * part] = wg_in[...]
    wall[mx, mz // STRIDE, mz % STRIDE, :, 2 * part : 3 * part] = wo_in[:, mine]

    groups = nz // STRIDE
    up = (groups + 1) // 2
    down = groups - 1 - up

    first_part = pl.ds(0, part)
    later_part = pl.ds(part, 2 * part + 128)

    def hop(direction, q):
        origin = (mz // STRIDE - direction * (q - 1) + groups) % groups
        ref = wall.at[mx, origin, mz % STRIDE]
        k = (q - 1) if direction > 0 else up + q - 1
        return pltpu.make_async_remote_copy(
            src_ref=ref, dst_ref=ref, send_sem=s_send.at[k], recv_sem=s_recv.at[k],
            device_id={"sp_1": (mz + direction * STRIDE + nz) % nz}, device_id_type=MESH,
        )

    def hop_in(q):
        hop(1, q).wait_recv()
        if q <= down:
            hop(-1, q).wait_recv()

    def hop_out(q):
        hop(1, q).start()
        if q <= down:
            hop(-1, q).start()

    def group_span(k):
        return ((0, groups), (0, groups), (groups // 2, groups), (0, groups // 2))[k]

    def piece(stage, k, g, count):
        step = (1, -1, 1, -1)[k]
        back_by = (0, 0, 1, -1)[k]
        if stage:
            lanes = (first_part, later_part)[stage - 1]
            ref = wall.at[(mx - back_by + nx) % nx, pl.ds(g, count), :, :, lanes]
            device = {"sp_0": (mx + step + nx) % nx}
        else:
            ref = wall.at[mx, pl.ds(g, count), (mz - back_by + nz) % STRIDE]
            device = {"sp_1": (mz + step + nz) % nz}
        return pltpu.make_async_remote_copy(
            src_ref=ref, dst_ref=ref, send_sem=r_send.at[stage, k], recv_sem=r_recv.at[stage, k],
            device_id=device, device_id_type=MESH,
        )

    def whole(stage, k):
        low, high = group_span(k)
        return piece(stage, k, low, high - low)

    def exchange(src, dst, send_sem, recv_sem, listen):
        def copy(i):
            device, target = partner(i)
            return pltpu.make_async_remote_copy(
                src_ref=src.at[target], dst_ref=dst.at[me],
                send_sem=send_sem.at[i], recv_sem=recv_sem.at[0],
                device_id=device, device_id_type=MESH,
            )

        def send(first, last):
            def body(i, carry):
                @pl.when(i >= WINDOW)
                def _():
                    copy(i - WINDOW).wait_send()

                if listen:

                    @pl.when(i % nx == 0)
                    def _():
                        _, target = partner(i)
                        hear(target % nz)

                copy(i).start()
                return carry

            lax.fori_loop(first, last, body, 0)

        def drain():
            def body(i, carry):
                copy(i).wait_send()
                return carry

            lax.fori_loop(n - 1 - WINDOW, n - 1, body, 0)
            some = dst.at[pl.ds(0, n - 1)]
            pltpu.make_async_copy(some, some, recv_sem.at[0]).wait()

        return send, drain

    send, drain = exchange(spread, arrived, a_send, a_recv, True)

    vocab = table.shape[1]
    low_count = 256
    high_count = vocab // low_count
    prompt = ids.shape[1]
    high_hot = one_hot(ids[...] // low_count == iota((high_count, prompt), 0))
    low_hot = one_hot(ids[...] % low_count == iota((low_count, prompt), 0))
    counts[...] = lax.dot_general(
        high_hot, low_hot, (((1,), (1,)), ((), ())), preferred_element_type=F32
    )

    def tally(h, total):
        piece = table[:, pl.ds(pl.multiple_of(h * low_count, low_count), low_count)]
        return total + piece.astype(F32) * counts[pl.ds(h, 1), :]

    few = table.shape[0]
    total = lax.fori_loop(0, high_count, tally, jnp.zeros((few, low_count), F32))
    pooled4 = jnp.sum(total, axis=1, keepdims=True) * (1.0 / prompt)
    pooled8 = jnp.concatenate([pooled4] * (block // few), axis=0)
    pooled8 = jnp.where(iota((block, 1), 0) // few == core, pooled8, 0.0)
    first = pooled8.astype(BF16).astype(F32)
    second = (pooled8 - first).astype(BF16).astype(F32)
    third = pooled8 - first - second
    lane = iota((block, 128), 1)
    terms = jnp.where(lane == 0, first, jnp.where(lane == 1, second, jnp.where(lane == 2, third, 0.0)))
    wall[mx, mz // STRIDE, mz % STRIDE, :, 3 * part : 3 * part + 128] = terms.astype(BF16)

    begin = jnp.where(mz < STRIDE, 28, 8)
    send(0, begin)
    pl.when(above > 0)(lambda: pl.semaphore_wait(ring_hello, above))
    hop_out(1)

    def send_pieces(stage, at, each, slack):
        for pair in ((0, 1), (2, 3)):
            count = group_span(pair[0])[1] - group_span(pair[0])[0]

            def body(g, carry, at=at, pair=pair):
                for k in pair:
                    piece(stage, k, group_span(k)[0] + g, 1).start()
                send(at + g * each, at + (g + 1) * each)
                return carry

            lax.fori_loop(0, count, body, 0)
            at += count * each
            send(at, at + slack)
            at += slack
            for k in pair:
                whole(stage, k).wait_recv()
        return at

    cells = TT * HH
    kt_wide = dot(kt[...], one_hot(iota((TT, cells), 1) // HH == iota((TT, cells), 0)))
    kh_wide = dot(kh[...], one_hot(iota((HH, cells), 1) % HH == iota((HH, cells), 0)))
    for s in range(TT):
        space[s * HH : (s + 1) * HH, :] = (kh_wide * kt_wide[s : s + 1, :]).astype(BF16)
    kw_wide = dot(kw[...], one_hot(iota((WW, rows), 1) // lines == iota((WW, rows), 0)))
    column_line = iota((WW, rows), 1) % lines
    for line in range(lines):
        wide[line * WW : (line + 1) * WW, :] = jnp.where(column_line == line, kw_wide, 0.0).astype(BF16)
    left_over = n - 1 - begin

    def until(share):
        return begin + left_over * share // 128

    done = begin
    for q in range(1, up + 1):
        send(done, until(11 * q))
        done = until(11 * q)
        hop_in(q)
        if q < up:
            hop_out(q + 1)
    share = 11 * up
    for stage in (0, 1):
        for pair in ((0, 1), (2, 3)):
            count = group_span(pair[0])[1] - group_span(pair[0])[0]
            for g in range(count):
                for k in pair:
                    piece(stage, k, group_span(k)[0] + g, 1).start()
                share += 1
                send(done, until(share))
                done = until(share)
            share += 7
            send(done, until(share))
            done = until(share)
            for k in pair:
                whole(stage, k).wait_recv()
    send(done, n - 1)
    drain()

    quarters = rows // tile
    ycopies = []
    for r in range(quarters):
        here = slice(r * tile, (r + 1) * tile)
        full = arrived[...].reshape(rows, part)
        y_own[here, :] = dot(space[here, :], full).astype(BF16)
        ycopies.append(pltpu.make_async_remote_copy(
            src_ref=y_own.at[pl.ds(r * tile, tile)], dst_ref=y_other.at[pl.ds(r * tile, tile)],
            send_sem=y_send.at[r], recv_sem=y_recv.at[r], device_id=other_core, device_id_type=MESH,
        ))
        ycopies[-1].start()
    gathered = wall.reshape(chans, 3 * part + 128)
    weight = gathered.at[:, 0:part]
    own_rows = pl.ds(pl.multiple_of(core * part, part), part)
    other_rows = pl.ds(pl.multiple_of((1 - core) * part, part), part)
    for r in range(quarters):
        here = slice(r * tile, (r + 1) * tile)
        ycopies[r].wait_recv()
        value = dot(y_own[here, :], weight[own_rows, :]) + dot(y_other[here, :], weight[other_rows, :])
        filt[here, :] = (value * spec[here, :].astype(F32)).astype(BF16)
    for r in range(quarters):
        here = slice(r * tile, (r + 1) * tile)
        got = dot(space[here, :], filt[...]).astype(BF16)
        back[r * per : (r + 1) * per] = got.reshape(per, block, part)
        ycopies[r].wait_send()
    returned[me] = back[me]
    send, drain = exchange(back, returned, b_send, b_recv, False)
    at = send_pieces(2, 0, 6, 16)
    send(at, n - 1)
    for q in range(1, up + 1):
        hop(1, q).wait_send()
        if q <= down:
            hop(-1, q).wait_send()
    for stage in range(3):
        for k in range(4):
            whole(stage, k).wait_send()

    upper = pl.ds(2 * part, part + 128)
    swap_out = pltpu.make_async_remote_copy(
        src_ref=wall.at[:, :, :, :, upper], dst_ref=wo_other, send_sem=o_send, recv_sem=o_recv,
        device_id=other_core, device_id_type=MESH,
    )
    swap_out.start()
    swap_out.wait()
    others = wo_other.reshape(chans, part + 128)
    pools = gathered[:, 3 * part : 3 * part + 128] + others[:, part : part + 128]
    chosen = one_hot(iota((chans, part), 0) == iota((chans, part), 1) + core * part)
    terms = lax.dot_general(pools, chosen, (((0,), (0,)), ((), ())), preferred_element_type=F32)
    modulation = 1.0 + jnp.sum(terms[0:8, :], axis=0, keepdims=True) + emb[...]

    def gate(r, carry):
        here = pl.ds(pl.multiple_of(r * tile, tile), tile)
        v = dot(lat[here, :], gathered[:, part : 2 * part])
        gain[here, :] = v / (1.0 + jnp.exp(-v)) * modulation
        return carry

    lax.fori_loop(0, quarters, gate, 0)
    drain()

    half = rows // 2

    def finish(r, dst, base):
        here = pl.ds(pl.multiple_of(base + r * tile, tile), tile)
        mix = dot(wide[here, :], returned[...].reshape(rows, part)) * gain[here, :]
        dst[pl.ds(pl.multiple_of(r * tile, tile), tile), :] = mix.astype(BF16)

    mcopies = []
    for r in range(half // tile):
        finish(r, spout, (1 - core) * half)
        mcopies.append(pltpu.make_async_remote_copy(
            src_ref=spout.at[pl.ds(r * tile, tile)], dst_ref=mix_other.at[pl.ds(r * tile, tile)],
            send_sem=m_send.at[r], recv_sem=m_recv.at[r], device_id=other_core, device_id_type=MESH,
        ))
        mcopies[-1].start()
    for r in range(half // tile):
        finish(r, mix_own, core * half)
    left = pl.ds(pl.multiple_of(core * part, part), part)
    right = pl.ds(pl.multiple_of((1 - core) * part, part), part)
    for r in range(half // tile):
        here = slice(r * tile, (r + 1) * tile)
        mcopies[r].wait()
        for at, weight in ((left, gathered.at[:, 2 * part : 3 * part]), (right, others.at[:, 0:part])):
            out[here, at] = dot(mix_own[here, :], weight[own_rows, :]) + dot(
                mix_other[here, :], weight[other_rows, :]
            )


def local(nx, nz, latents, spectrum, w_value, w_gate, w_out, embed_table, prompt_ids, noise_step):
    rows, chans = latents.shape
    block, part = w_value.shape
    n = nx * nz
    core = lax.axis_index("ch")
    channel = core * part + jnp.arange(part, dtype=jnp.int32)
    emb = step_embedding(noise_step, channel, chans).reshape(1, part)
    half = rows // 2
    groups = nz // STRIDE
    hops = groups - 1
    vmem = pl.BlockSpec(memory_space=pltpu.VMEM)
    dma = pltpu.SemaphoreType.DMA
    exchanged = pltpu.VMEM((n, rows // n, part), BF16)
    plain = pltpu.VMEM((rows, part), BF16)
    summed = pl.pallas_call(
        functools.partial(kernel, nx, nz),
        out_shape=jax.ShapeDtypeStruct((half, chans), F32),
        in_specs=[vmem] * 11,
        out_specs=vmem,
        scratch_shapes=[
            exchanged, exchanged,
            pltpu.VMEM((8, 128), BF16), pltpu.VMEM((half, part), BF16),
            exchanged, exchanged,
            plain, plain, plain,
            pltpu.VMEM((rows, part), F32),
            pltpu.VMEM((nx, groups, STRIDE, block, 3 * part + 128), BF16),
            pltpu.VMEM((nx, groups, STRIDE, block, part + 128), BF16),
            pltpu.VMEM((half, part), BF16), pltpu.VMEM((half, part), BF16),
            pltpu.VMEM((embed_table.shape[1] // 256, 256), F32),
            pltpu.VMEM((rows, rows), BF16), pltpu.VMEM((rows, rows), BF16), pltpu.VMEM((rows, rows), BF16),
            pltpu.SemaphoreType.REGULAR((nz,)), pltpu.SemaphoreType.REGULAR, dma((n,)), dma((1,)), dma((n,)), dma((1,)),
            dma((hops,)), dma((hops,)), dma((3, 4)), dma((3, 4)),
            dma((4,)), dma((4,)), dma, dma, dma((2,)), dma((2,)),
        ],
        compiler_params=pltpu.CompilerParams(
            collective_id=0, has_side_effects=True, vmem_limit_bytes=56 * 2**20
        ),
    )(
        latents, spectrum.reshape(rows, part), w_value, w_gate, w_out, embed_table,
        prompt_ids.reshape(1, -1), emb, cas_table(WW), cas_table(HH), cas_table(TT),
    )
    residual = lax.dynamic_slice_in_dim(latents, core * half, half, 0)
    return (residual.astype(F32) + summed).astype(BF16)


def solution(mesh):
    nx, nz = 4, mesh.shape["sp"] // 4
    torus = Mesh(
        mesh.devices.reshape(mesh.shape["grp"], nx, nz, mesh.shape["ch"]),
        ("grp", "sp_0", "sp_1", "ch"),
    )
    in_specs = (
        P(GRP_SP, None),
        P(None, None, SP, "ch"),
        P(SP, "ch"),
        P(SP, "ch"),
        P(SP, None),
        P(SP_CH, None),
        P("grp"),
        P("grp"),
    )
    out_specs = P(GRP_SP_CH, None)
    return jax.shard_map(
        functools.partial(local, nx, nz),
        mesh=torus, in_specs=in_specs, out_specs=out_specs, check_vma=False,
    )
```

```python
import functools
import math

import jax
import jax.numpy as jnp
import numpy as np
from jax import lax
from jax.experimental import pallas as pl
from jax.experimental.pallas import tpu as pltpu
from jax.sharding import Mesh
from jax.sharding import PartitionSpec as P

TT = 16
HH = 64
WW = 128
SP_CH = ("sp_0", "sp_1", "ch")
GRP_SP = ("grp", "sp_0", "sp_1")
GRP_SP_CH = ("grp", "sp_0", "sp_1", "ch")
SP = ("sp_0", "sp_1")
F32 = jnp.float32
BF16 = jnp.bfloat16
MESH = pl.DeviceIdType.MESH
STRIDE = 4
WINDOW = 40


def cas_table(length):
    position = np.arange(length, dtype=np.int32)
    product = position[:, None] * position[None, :] % length
    phase_angle = product.astype(np.float32) * np.float32(2.0 * math.pi / length)
    table = (np.cos(phase_angle) + np.sin(phase_angle)) / np.float32(math.sqrt(length))
    return jnp.asarray(table.astype(jnp.bfloat16))


def step_embedding(noise_step, channel, channels):
    half_count = channels // 2
    lower_half = channel < half_count
    position = jnp.where(lower_half, channel, channel - half_count).astype(jnp.float32)
    frequency = jnp.exp(-math.log(10000.0) * position / half_count)
    phase_angle = noise_step[0].astype(jnp.float32) * frequency
    return jnp.where(lower_half, jnp.sin(phase_angle), jnp.cos(phase_angle))


def dot(a, b):
    return jnp.dot(a, b, preferred_element_type=F32)


def iota(shape, dim):
    return lax.broadcasted_iota(jnp.int32, shape, dim)


def one_hot(condition):
    return jnp.where(condition, 1.0, 0.0).astype(BF16)


def kernel(
    nx, nz,
    lat, spec, wv_in, wg_in, wo_in, table, ids, emb, kw, kh, kt,
    out,
    spread, arrived, spin, spout, back, returned, y_own, y_other, filt, gain,
    wall, wo_other, mix_own, mix_other, counts, space, wide, narrow,
    a_send, a_recv, b_send, b_recv, s_send, s_recv, r_send, r_recv,
    y_send, y_recv, o_send, o_recv, m_send, m_recv,
):
    n = nx * nz
    rows, chans = lat.shape
    part = wv_in.shape[1]
    lines = rows // WW
    block = rows // n
    mx, mz, core = lax.axis_index("sp_0"), lax.axis_index("sp_1"), lax.axis_index("ch")
    me = mx * nz + mz
    other_core = {"ch": 1 - core}

    def partner(i):
        j = n - 1 - i
        zi, dx = j // nx, j % nx
        m = (zi + 1) // 2
        dz = jnp.where(zi % 2 == 1, m, nz - m) % nz
        tx, tz = (mx + dx) % nx, (mz + dz) % nz
        return {"sp_0": tx, "sp_1": tz}, tx * nz + tz

    barrier = pltpu.get_barrier_semaphore()

    def greet(i, carry):
        device, _ = partner(i)
        pl.semaphore_signal(barrier, inc=1, device_id=device, device_id_type=MESH)
        return carry

    lax.fori_loop(0, n - 1, greet, 0)
    pl.semaphore_signal(barrier, inc=1, device_id=other_core, device_id_type=MESH)

    pick = one_hot(iota((rows, WW), 0) // lines == iota((rows, WW), 1))
    spread_rows = dot(pick, kw[...]).astype(BF16)
    line_of = iota((rows, WW), 0) % lines
    for line in range(lines):
        narrow[:, line * WW : (line + 1) * WW] = jnp.where(
            line_of == line, spread_rows, jnp.zeros_like(spread_rows)
        )
    mine = pl.ds(pl.multiple_of(core * part, 128), part)
    tile = 256
    per = tile // block

    def widen(r, carry):
        at = pl.ds(pl.multiple_of(r * tile, tile), tile)
        got = dot(narrow[at, :], lat[:, mine]).astype(BF16)
        spread[pl.ds(r * per, per)] = got.reshape(per, block, part)
        return carry

    lax.fori_loop(0, rows // tile, widen, 0)
    arrived[me] = spread[me]
    wall[mx, mz // STRIDE, mz % STRIDE, :, 0:part] = wv_in[...]
    wall[mx, mz // STRIDE, mz % STRIDE, :, part : 2 * part] = wg_in[...]
    wall[mx, mz // STRIDE, mz % STRIDE, :, 2 * part : 3 * part] = wo_in[:, mine]

    pl.semaphore_wait(barrier, n)

    groups = nz // STRIDE
    up = (groups + 1) // 2
    down = groups - 1 - up

    first_part = pl.ds(0, part)
    later_part = pl.ds(part, 2 * part + 128)

    def hop(stream, direction, q):
        origin = (mz // STRIDE - direction * (q - 1) + groups) % groups
        ref = wall.at[mx, origin, mz % STRIDE, :, (first_part, later_part)[stream]]
        k = (q - 1) if direction > 0 else up + q - 1
        return pltpu.make_async_remote_copy(
            src_ref=ref, dst_ref=ref, send_sem=s_send.at[stream, k], recv_sem=s_recv.at[stream, k],
            device_id={"sp_1": (mz + direction * STRIDE + nz) % nz}, device_id_type=MESH,
        )

    def hop_in(stream, q):
        hop(stream, 1, q).wait_recv()
        if q <= down:
            hop(stream, -1, q).wait_recv()

    def hop_out(stream, q):
        hop(stream, 1, q).start()
        if q <= down:
            hop(stream, -1, q).start()

    def group_span(k):
        return ((0, groups), (0, groups), (groups // 2, groups), (0, groups // 2))[k]

    def piece(stage, k, g, count):
        step = (1, -1, 1, -1)[k]
        back_by = (0, 0, 1, -1)[k]
        lanes = (first_part, later_part)[stage // 2]
        if stage % 2:
            ref = wall.at[(mx - back_by + nx) % nx, pl.ds(g, count), :, :, lanes]
            device = {"sp_0": (mx + step + nx) % nx}
        else:
            ref = wall.at[mx, pl.ds(g, count), (mz - back_by + nz) % STRIDE, :, lanes]
            device = {"sp_1": (mz + step + nz) % nz}
        return pltpu.make_async_remote_copy(
            src_ref=ref, dst_ref=ref, send_sem=r_send.at[stage, k], recv_sem=r_recv.at[stage, k],
            device_id=device, device_id_type=MESH,
        )

    def whole(stage, k):
        low, high = group_span(k)
        return piece(stage, k, low, high - low)

    def exchange(src, dst, send_sem, recv_sem):
        def copy(i):
            device, target = partner(i)
            return pltpu.make_async_remote_copy(
                src_ref=src.at[target], dst_ref=dst.at[me],
                send_sem=send_sem.at[i], recv_sem=recv_sem.at[0],
                device_id=device, device_id_type=MESH,
            )

        def send(first, last):
            def body(i, carry):
                @pl.when(i >= WINDOW)
                def _():
                    copy(i - WINDOW).wait_send()

                copy(i).start()
                return carry

            lax.fori_loop(first, last, body, 0)

        def drain():
            def body(i, carry):
                copy(i).wait_send()
                return carry

            lax.fori_loop(n - 1 - WINDOW, n - 1, body, 0)
            some = dst.at[pl.ds(0, n - 1)]
            pltpu.make_async_copy(some, some, recv_sem.at[0]).wait()

        return send, drain

    send, drain = exchange(spread, arrived, a_send, a_recv)
    hop_out(0, 1)
    send(0, 8)

    vocab = table.shape[1]
    low_count = 256
    high_count = vocab // low_count
    prompt = ids.shape[1]
    high_hot = one_hot(ids[...] // low_count == iota((high_count, prompt), 0))
    low_hot = one_hot(ids[...] % low_count == iota((low_count, prompt), 0))
    counts[...] = lax.dot_general(
        high_hot, low_hot, (((1,), (1,)), ((), ())), preferred_element_type=F32
    )

    def tally(h, total):
        piece = table[:, pl.ds(pl.multiple_of(h * low_count, low_count), low_count)]
        return total + piece.astype(F32) * counts[pl.ds(h, 1), :]

    few = table.shape[0]
    total = lax.fori_loop(0, high_count, tally, jnp.zeros((few, low_count), F32))
    pooled4 = jnp.sum(total, axis=1, keepdims=True) * (1.0 / prompt)
    pooled8 = jnp.concatenate([pooled4] * (block // few), axis=0)
    pooled8 = jnp.where(iota((block, 1), 0) // few == core, pooled8, 0.0)
    first = pooled8.astype(BF16).astype(F32)
    second = (pooled8 - first).astype(BF16).astype(F32)
    third = pooled8 - first - second
    lane = iota((block, 128), 1)
    terms = jnp.where(lane == 0, first, jnp.where(lane == 1, second, jnp.where(lane == 2, third, 0.0)))
    wall[mx, mz // STRIDE, mz % STRIDE, :, 3 * part : 3 * part + 128] = terms.astype(BF16)

    def send_hops(at, pace):
        for q in range(1, up + 1):
            send(at, at + pace)
            at += pace
            hop_in(0, q)
            if q < up:
                hop_out(0, q + 1)
        return at

    def send_pieces(stage, at, each, slack):
        for pair in ((0, 1), (2, 3)):
            count = group_span(pair[0])[1] - group_span(pair[0])[0]

            def body(g, carry, at=at, pair=pair):
                for k in pair:
                    piece(stage, k, group_span(k)[0] + g, 1).start()
                send(at + g * each, at + (g + 1) * each)
                return carry

            lax.fori_loop(0, count, body, 0)
            at += count * each
            send(at, at + slack)
            at += slack
            for k in pair:
                whole(stage, k).wait_recv()
        return at

    cells = TT * HH
    kt_wide = dot(kt[...], one_hot(iota((TT, cells), 1) // HH == iota((TT, cells), 0)))
    kh_wide = dot(kh[...], one_hot(iota((HH, cells), 1) % HH == iota((HH, cells), 0)))
    for s in range(TT):
        space[s * HH : (s + 1) * HH, :] = (kh_wide * kt_wide[s : s + 1, :]).astype(BF16)
    kw_wide = dot(kw[...], one_hot(iota((WW, rows), 1) // lines == iota((WW, rows), 0)))
    column_line = iota((WW, rows), 1) % lines
    for line in range(lines):
        wide[line * WW : (line + 1) * WW, :] = jnp.where(column_line == line, kw_wide, 0.0).astype(BF16)
    at = send_hops(8, 13)
    at = send_pieces(0, at, 1, 8)
    at = send_pieces(1, at, 1, 8)
    send(at, n - 1)
    drain()

    quarters = rows // tile
    gathered = wall.reshape(chans, 3 * part + 128)
    value_weight = gathered.at[:, 0:part]
    own_rows = pl.ds(pl.multiple_of(core * part, part), part)
    other_rows = pl.ds(pl.multiple_of((1 - core) * part, part), part)
    ycopies = [
        pltpu.make_async_remote_copy(
            src_ref=y_own.at[pl.ds(r * tile, tile)], dst_ref=y_other.at[pl.ds(r * tile, tile)],
            send_sem=y_send.at[r], recv_sem=y_recv.at[r], device_id=other_core, device_id_type=MESH,
        )
        for r in range(quarters)
    ]

    def forward(r):
        here = slice(r * tile, (r + 1) * tile)
        y_own[here, :] = dot(space[here, :], arrived[...].reshape(rows, part)).astype(BF16)
        ycopies[r].start()

    def project(r):
        here = slice(r * tile, (r + 1) * tile)
        ycopies[r].wait_recv()
        value = dot(y_own[here, :], value_weight[own_rows, :])
        value = value + dot(y_other[here, :], value_weight[other_rows, :])
        filt[here, :] = (value * spec[here, :].astype(F32)).astype(BF16)

    def backward(r):
        here = slice(r * tile, (r + 1) * tile)
        got = dot(space[here, :], filt[...]).astype(BF16)
        back[r * per : (r + 1) * per] = got.reshape(per, block, part)
        ycopies[r].wait_send()

    def chain(step):
        if 0 < step <= up:
            hop_in(1, step)
        if step < up:
            hop_out(1, step + 1)
        if step == up:
            whole(2, 0).start()
            whole(2, 1).start()
        if step == up + 1:
            whole(2, 0).wait_recv()
            whole(2, 1).wait_recv()
            whole(2, 2).start()
            whole(2, 3).start()

    work = [functools.partial(f, r) for f in (forward, project, backward) for r in range(quarters)]
    for at, piece_of_work in enumerate(work):
        if at % 2 == 0:
            chain(at // 2)
        piece_of_work()
    returned[me] = back[me]
    send, drain = exchange(back, returned, b_send, b_recv)
    send(0, 16)
    whole(2, 2).wait_recv()
    whole(2, 3).wait_recv()
    at = send_pieces(3, 16, 5, 16)
    send(at, n - 1)
    for stream in range(2):
        for q in range(1, up + 1):
            hop(stream, 1, q).wait_send()
            if q <= down:
                hop(stream, -1, q).wait_send()
    for stage in range(4):
        for k in range(4):
            whole(stage, k).wait_send()

    upper = pl.ds(2 * part, part + 128)
    swap_out = pltpu.make_async_remote_copy(
        src_ref=wall.at[:, :, :, :, upper], dst_ref=wo_other, send_sem=o_send, recv_sem=o_recv,
        device_id=other_core, device_id_type=MESH,
    )
    swap_out.start()
    swap_out.wait()
    others = wo_other.reshape(chans, part + 128)
    pools = gathered[:, 3 * part : 3 * part + 128] + others[:, part : part + 128]
    chosen = one_hot(iota((chans, part), 0) == iota((chans, part), 1) + core * part)
    terms = lax.dot_general(pools, chosen, (((0,), (0,)), ((), ())), preferred_element_type=F32)
    modulation = 1.0 + jnp.sum(terms[0:8, :], axis=0, keepdims=True) + emb[...]

    def gate(r, carry):
        here = pl.ds(pl.multiple_of(r * tile, tile), tile)
        v = dot(lat[here, :], gathered[:, part : 2 * part])
        gain[here, :] = v / (1.0 + jnp.exp(-v)) * modulation
        return carry

    lax.fori_loop(0, quarters, gate, 0)
    drain()

    half = rows // 2

    def finish(r, dst, base):
        here = pl.ds(pl.multiple_of(base + r * tile, tile), tile)
        mix = dot(wide[here, :], returned[...].reshape(rows, part)) * gain[here, :]
        dst[pl.ds(pl.multiple_of(r * tile, tile), tile), :] = mix.astype(BF16)

    mcopies = []
    for r in range(half // tile):
        finish(r, spout, (1 - core) * half)
        mcopies.append(pltpu.make_async_remote_copy(
            src_ref=spout.at[pl.ds(r * tile, tile)], dst_ref=mix_other.at[pl.ds(r * tile, tile)],
            send_sem=m_send.at[r], recv_sem=m_recv.at[r], device_id=other_core, device_id_type=MESH,
        ))
        mcopies[-1].start()
    for r in range(half // tile):
        finish(r, mix_own, core * half)
    left = pl.ds(pl.multiple_of(core * part, part), part)
    right = pl.ds(pl.multiple_of((1 - core) * part, part), part)
    for r in range(half // tile):
        here = slice(r * tile, (r + 1) * tile)
        mcopies[r].wait()
        for at, weight in ((left, gathered.at[:, 2 * part : 3 * part]), (right, others.at[:, 0:part])):
            out[here, at] = dot(mix_own[here, :], weight[own_rows, :]) + dot(
                mix_other[here, :], weight[other_rows, :]
            )


def local(nx, nz, latents, spectrum, w_value, w_gate, w_out, embed_table, prompt_ids, noise_step):
    rows, chans = latents.shape
    block, part = w_value.shape
    n = nx * nz
    core = lax.axis_index("ch")
    channel = core * part + jnp.arange(part, dtype=jnp.int32)
    emb = step_embedding(noise_step, channel, chans).reshape(1, part)
    half = rows // 2
    groups = nz // STRIDE
    hops = groups - 1
    vmem = pl.BlockSpec(memory_space=pltpu.VMEM)
    dma = pltpu.SemaphoreType.DMA
    exchanged = pltpu.VMEM((n, rows // n, part), BF16)
    plain = pltpu.VMEM((rows, part), BF16)
    summed = pl.pallas_call(
        functools.partial(kernel, nx, nz),
        out_shape=jax.ShapeDtypeStruct((half, chans), F32),
        in_specs=[vmem] * 11,
        out_specs=vmem,
        scratch_shapes=[
            exchanged, exchanged,
            pltpu.VMEM((8, 128), BF16), pltpu.VMEM((half, part), BF16),
            exchanged, exchanged,
            plain, plain, plain,
            pltpu.VMEM((rows, part), F32),
            pltpu.VMEM((nx, groups, STRIDE, block, 3 * part + 128), BF16),
            pltpu.VMEM((nx, groups, STRIDE, block, part + 128), BF16),
            pltpu.VMEM((half, part), BF16), pltpu.VMEM((half, part), BF16),
            pltpu.VMEM((embed_table.shape[1] // 256, 256), F32),
            pltpu.VMEM((rows, rows), BF16), pltpu.VMEM((rows, rows), BF16), pltpu.VMEM((rows, rows), BF16),
            dma((n,)), dma((1,)), dma((n,)), dma((1,)),
            dma((2, hops)), dma((2, hops)), dma((4, 4)), dma((4, 4)),
            dma((4,)), dma((4,)), dma, dma, dma((2,)), dma((2,)),
        ],
        compiler_params=pltpu.CompilerParams(
            collective_id=0, has_side_effects=True, vmem_limit_bytes=56 * 2**20
        ),
    )(
        latents, spectrum.reshape(rows, part), w_value, w_gate, w_out, embed_table,
        prompt_ids.reshape(1, -1), emb, cas_table(WW), cas_table(HH), cas_table(TT),
    )
    residual = lax.dynamic_slice_in_dim(latents, core * half, half, 0)
    return (residual.astype(F32) + summed).astype(BF16)


def solution(mesh):
    nx, nz = 4, mesh.shape["sp"] // 4
    torus = Mesh(
        mesh.devices.reshape(mesh.shape["grp"], nx, nz, mesh.shape["ch"]),
        ("grp", "sp_0", "sp_1", "ch"),
    )
    in_specs = (
        P(GRP_SP, None),
        P(None, None, SP, "ch"),
        P(SP, "ch"),
        P(SP, "ch"),
        P(SP, None),
        P(SP_CH, None),
        P("grp"),
        P("grp"),
    )
    out_specs = P(GRP_SP_CH, None)
    return jax.shard_map(
        functools.partial(local, nx, nz),
        mesh=torus, in_specs=in_specs, out_specs=out_specs, check_vma=False,
    )
```

```python
import functools
import math

import jax
import jax.numpy as jnp
import numpy as np
from jax import lax
from jax.experimental import pallas as pl
from jax.experimental.pallas import tpu as pltpu
from jax.sharding import Mesh
from jax.sharding import PartitionSpec as P

TT = 16
HH = 64
WW = 128
SP_CH = ("sp_0", "sp_1", "ch")
GRP_SP = ("grp", "sp_0", "sp_1")
GRP_SP_CH = ("grp", "sp_0", "sp_1", "ch")
SP = ("sp_0", "sp_1")
F32 = jnp.float32
BF16 = jnp.bfloat16
MESH = pl.DeviceIdType.MESH
STRIDE = 4
WINDOW = 40


def cas_table(length):
    position = np.arange(length, dtype=np.int32)
    product = position[:, None] * position[None, :] % length
    phase_angle = product.astype(np.float32) * np.float32(2.0 * math.pi / length)
    table = (np.cos(phase_angle) + np.sin(phase_angle)) / np.float32(math.sqrt(length))
    return jnp.asarray(table.astype(jnp.bfloat16))


def step_embedding(noise_step, channel, channels):
    half_count = channels // 2
    lower_half = channel < half_count
    position = jnp.where(lower_half, channel, channel - half_count).astype(jnp.float32)
    frequency = jnp.exp(-math.log(10000.0) * position / half_count)
    phase_angle = noise_step[0].astype(jnp.float32) * frequency
    return jnp.where(lower_half, jnp.sin(phase_angle), jnp.cos(phase_angle))


def dot(a, b):
    return jnp.dot(a, b, preferred_element_type=F32)


def iota(shape, dim):
    return lax.broadcasted_iota(jnp.int32, shape, dim)


def one_hot(condition):
    return jnp.where(condition, 1.0, 0.0).astype(BF16)


def kernel(
    nx, nz,
    lat, spec, wv_in, wg_in, wo_in, table, ids, emb, kw, kh, kt,
    out,
    spread, arrived, spin, spout, back, returned, y_own, y_other, filt, gain,
    wall, wo_other, mix_own, mix_other, counts, space, wide, narrow,
    a_send, a_recv, b_send, b_recv, s_send, s_recv, r_send, r_recv,
    y_send, y_recv, o_send, o_recv, m_send, m_recv,
):
    n = nx * nz
    rows, chans = lat.shape
    part = wv_in.shape[1]
    lines = rows // WW
    block = rows // n
    mx, mz, core = lax.axis_index("sp_0"), lax.axis_index("sp_1"), lax.axis_index("ch")
    me = mx * nz + mz
    other_core = {"ch": 1 - core}

    def partner(i):
        j = n - 1 - i
        zi, dx = j // nx, j % nx
        m = (zi + 1) // 2
        dz = jnp.where(zi % 2 == 1, m, nz - m) % nz
        tx, tz = (mx + dx) % nx, (mz + dz) % nz
        return {"sp_0": tx, "sp_1": tz}, tx * nz + tz

    barrier = pltpu.get_barrier_semaphore()

    def greet(i, carry):
        device, _ = partner(i)
        pl.semaphore_signal(barrier, inc=1, device_id=device, device_id_type=MESH)
        return carry

    lax.fori_loop(0, n - 1, greet, 0)
    pl.semaphore_signal(barrier, inc=1, device_id=other_core, device_id_type=MESH)

    pick = one_hot(iota((rows, WW), 0) // lines == iota((rows, WW), 1))
    spread_rows = dot(pick, kw[...]).astype(BF16)
    line_of = iota((rows, WW), 0) % lines
    for line in range(lines):
        narrow[:, line * WW : (line + 1) * WW] = jnp.where(
            line_of == line, spread_rows, jnp.zeros_like(spread_rows)
        )
    mine = pl.ds(pl.multiple_of(core * part, 128), part)
    tile = 256
    per = tile // block

    def widen(r, carry):
        at = pl.ds(pl.multiple_of(r * tile, tile), tile)
        got = dot(narrow[at, :], lat[:, mine]).astype(BF16)
        spread[pl.ds(r * per, per)] = got.reshape(per, block, part)
        return carry

    lax.fori_loop(0, rows // tile, widen, 0)
    arrived[me] = spread[me]
    wall[mx, mz // STRIDE, mz % STRIDE, :, 0:part] = wv_in[...]
    wall[mx, mz // STRIDE, mz % STRIDE, :, part : 2 * part] = wg_in[...]
    wall[mx, mz // STRIDE, mz % STRIDE, :, 2 * part : 3 * part] = wo_in[:, mine]

    pl.semaphore_wait(barrier, n)

    groups = nz // STRIDE
    up = (groups + 1) // 2
    down = groups - 1 - up

    first_part = pl.ds(0, part)
    later_part = pl.ds(part, 2 * part + 128)

    def hop(direction, q):
        origin = (mz // STRIDE - direction * (q - 1) + groups) % groups
        ref = wall.at[mx, origin, mz % STRIDE]
        k = (q - 1) if direction > 0 else up + q - 1
        return pltpu.make_async_remote_copy(
            src_ref=ref, dst_ref=ref, send_sem=s_send.at[k], recv_sem=s_recv.at[k],
            device_id={"sp_1": (mz + direction * STRIDE + nz) % nz}, device_id_type=MESH,
        )

    def hop_in(q):
        hop(1, q).wait_recv()
        if q <= down:
            hop(-1, q).wait_recv()

    def hop_out(q):
        hop(1, q).start()
        if q <= down:
            hop(-1, q).start()

    def group_span(k):
        return ((0, groups), (0, groups), (groups // 2, groups), (0, groups // 2))[k]

    def piece(stage, k, g, count):
        step = (1, -1, 1, -1)[k]
        back_by = (0, 0, 1, -1)[k]
        lanes = (first_part, later_part)[stage // 2]
        if stage % 2:
            ref = wall.at[(mx - back_by + nx) % nx, pl.ds(g, count), :, :, lanes]
            device = {"sp_0": (mx + step + nx) % nx}
        else:
            ref = wall.at[mx, pl.ds(g, count), (mz - back_by + nz) % STRIDE, :, lanes]
            device = {"sp_1": (mz + step + nz) % nz}
        return pltpu.make_async_remote_copy(
            src_ref=ref, dst_ref=ref, send_sem=r_send.at[stage, k], recv_sem=r_recv.at[stage, k],
            device_id=device, device_id_type=MESH,
        )

    def whole(stage, k):
        low, high = group_span(k)
        return piece(stage, k, low, high - low)

    def exchange(src, dst, send_sem, recv_sem):
        def copy(i):
            device, target = partner(i)
            return pltpu.make_async_remote_copy(
                src_ref=src.at[target], dst_ref=dst.at[me],
                send_sem=send_sem.at[i], recv_sem=recv_sem.at[0],
                device_id=device, device_id_type=MESH,
            )

        def send(first, last):
            def body(i, carry):
                @pl.when(i >= WINDOW)
                def _():
                    copy(i - WINDOW).wait_send()

                copy(i).start()
                return carry

            lax.fori_loop(first, last, body, 0)

        def drain():
            def body(i, carry):
                copy(i).wait_send()
                return carry

            lax.fori_loop(n - 1 - WINDOW, n - 1, body, 0)
            some = dst.at[pl.ds(0, n - 1)]
            pltpu.make_async_copy(some, some, recv_sem.at[0]).wait()

        return send, drain

    send, drain = exchange(spread, arrived, a_send, a_recv)
    send(0, 8)

    vocab = table.shape[1]
    low_count = 256
    high_count = vocab // low_count
    prompt = ids.shape[1]
    high_hot = one_hot(ids[...] // low_count == iota((high_count, prompt), 0))
    low_hot = one_hot(ids[...] % low_count == iota((low_count, prompt), 0))
    counts[...] = lax.dot_general(
        high_hot, low_hot, (((1,), (1,)), ((), ())), preferred_element_type=F32
    )

    def tally(h, total):
        piece = table[:, pl.ds(pl.multiple_of(h * low_count, low_count), low_count)]
        return total + piece.astype(F32) * counts[pl.ds(h, 1), :]

    few = table.shape[0]
    total = lax.fori_loop(0, high_count, tally, jnp.zeros((few, low_count), F32))
    pooled4 = jnp.sum(total, axis=1, keepdims=True) * (1.0 / prompt)
    pooled8 = jnp.concatenate([pooled4] * (block // few), axis=0)
    pooled8 = jnp.where(iota((block, 1), 0) // few == core, pooled8, 0.0)
    first = pooled8.astype(BF16).astype(F32)
    second = (pooled8 - first).astype(BF16).astype(F32)
    third = pooled8 - first - second
    lane = iota((block, 128), 1)
    terms = jnp.where(lane == 0, first, jnp.where(lane == 1, second, jnp.where(lane == 2, third, 0.0)))
    wall[mx, mz // STRIDE, mz % STRIDE, :, 3 * part : 3 * part + 128] = terms.astype(BF16)
    hop_out(1)

    def send_hops(at, pace):
        for q in range(1, up + 1):
            send(at, at + pace)
            at += pace
            hop_in(q)
            if q < up:
                hop_out(q + 1)
        return at

    def send_pieces(stage, at, each, slack):
        for pair in ((0, 1), (2, 3)):
            count = group_span(pair[0])[1] - group_span(pair[0])[0]

            def body(g, carry, at=at, pair=pair):
                for k in pair:
                    piece(stage, k, group_span(k)[0] + g, 1).start()
                send(at + g * each, at + (g + 1) * each)
                return carry

            lax.fori_loop(0, count, body, 0)
            at += count * each
            send(at, at + slack)
            at += slack
            for k in pair:
                whole(stage, k).wait_recv()
        return at

    cells = TT * HH
    kt_wide = dot(kt[...], one_hot(iota((TT, cells), 1) // HH == iota((TT, cells), 0)))
    kh_wide = dot(kh[...], one_hot(iota((HH, cells), 1) % HH == iota((HH, cells), 0)))
    for s in range(TT):
        space[s * HH : (s + 1) * HH, :] = (kh_wide * kt_wide[s : s + 1, :]).astype(BF16)
    kw_wide = dot(kw[...], one_hot(iota((WW, rows), 1) // lines == iota((WW, rows), 0)))
    column_line = iota((WW, rows), 1) % lines
    for line in range(lines):
        wide[line * WW : (line + 1) * WW, :] = jnp.where(column_line == line, kw_wide, 0.0).astype(BF16)
    at = send_hops(8, 13)
    at = send_pieces(0, at, 1, 8)
    at = send_pieces(1, at, 1, 8)
    send(at, n - 1)
    drain()

    quarters = rows // tile
    gathered = wall.reshape(chans, 3 * part + 128)
    value_weight = gathered.at[:, 0:part]
    own_rows = pl.ds(pl.multiple_of(core * part, part), part)
    other_rows = pl.ds(pl.multiple_of((1 - core) * part, part), part)
    ycopies = [
        pltpu.make_async_remote_copy(
            src_ref=y_own.at[pl.ds(r * tile, tile)], dst_ref=y_other.at[pl.ds(r * tile, tile)],
            send_sem=y_send.at[r], recv_sem=y_recv.at[r], device_id=other_core, device_id_type=MESH,
        )
        for r in range(quarters)
    ]

    def forward(r):
        here = slice(r * tile, (r + 1) * tile)
        y_own[here, :] = dot(space[here, :], arrived[...].reshape(rows, part)).astype(BF16)
        ycopies[r].start()

    def project(r):
        here = slice(r * tile, (r + 1) * tile)
        ycopies[r].wait_recv()
        value = dot(y_own[here, :], value_weight[own_rows, :])
        value = value + dot(y_other[here, :], value_weight[other_rows, :])
        filt[here, :] = (value * spec[here, :].astype(F32)).astype(BF16)

    def backward(r):
        here = slice(r * tile, (r + 1) * tile)
        got = dot(space[here, :], filt[...]).astype(BF16)
        back[r * per : (r + 1) * per] = got.reshape(per, block, part)
        ycopies[r].wait_send()

    work = [functools.partial(f, r) for f in (forward, project, backward) for r in range(quarters)]
    for at, piece_of_work in enumerate(work):
        if at == 0:
            whole(2, 0).start()
            whole(2, 1).start()
        if at == 2 * quarters:
            whole(2, 0).wait_recv()
            whole(2, 1).wait_recv()
            whole(2, 2).start()
            whole(2, 3).start()
        piece_of_work()
    returned[me] = back[me]
    send, drain = exchange(back, returned, b_send, b_recv)
    send(0, 16)
    whole(2, 2).wait_recv()
    whole(2, 3).wait_recv()
    at = send_pieces(3, 16, 5, 16)
    send(at, n - 1)
    for q in range(1, up + 1):
        hop(1, q).wait_send()
        if q <= down:
            hop(-1, q).wait_send()
    for stage in range(4):
        for k in range(4):
            whole(stage, k).wait_send()

    upper = pl.ds(2 * part, part + 128)
    swap_out = pltpu.make_async_remote_copy(
        src_ref=wall.at[:, :, :, :, upper], dst_ref=wo_other, send_sem=o_send, recv_sem=o_recv,
        device_id=other_core, device_id_type=MESH,
    )
    swap_out.start()
    swap_out.wait()
    others = wo_other.reshape(chans, part + 128)
    pools = gathered[:, 3 * part : 3 * part + 128] + others[:, part : part + 128]
    chosen = one_hot(iota((chans, part), 0) == iota((chans, part), 1) + core * part)
    terms = lax.dot_general(pools, chosen, (((0,), (0,)), ((), ())), preferred_element_type=F32)
    modulation = 1.0 + jnp.sum(terms[0:8, :], axis=0, keepdims=True) + emb[...]

    def gate(r, carry):
        here = pl.ds(pl.multiple_of(r * tile, tile), tile)
        v = dot(lat[here, :], gathered[:, part : 2 * part])
        gain[here, :] = v / (1.0 + jnp.exp(-v)) * modulation
        return carry

    lax.fori_loop(0, quarters, gate, 0)
    drain()

    half = rows // 2

    def finish(r, dst, base):
        here = pl.ds(pl.multiple_of(base + r * tile, tile), tile)
        mix = dot(wide[here, :], returned[...].reshape(rows, part)) * gain[here, :]
        dst[pl.ds(pl.multiple_of(r * tile, tile), tile), :] = mix.astype(BF16)

    mcopies = []
    for r in range(half // tile):
        finish(r, spout, (1 - core) * half)
        mcopies.append(pltpu.make_async_remote_copy(
            src_ref=spout.at[pl.ds(r * tile, tile)], dst_ref=mix_other.at[pl.ds(r * tile, tile)],
            send_sem=m_send.at[r], recv_sem=m_recv.at[r], device_id=other_core, device_id_type=MESH,
        ))
        mcopies[-1].start()
    for r in range(half // tile):
        finish(r, mix_own, core * half)
    left = pl.ds(pl.multiple_of(core * part, part), part)
    right = pl.ds(pl.multiple_of((1 - core) * part, part), part)
    for r in range(half // tile):
        here = slice(r * tile, (r + 1) * tile)
        mcopies[r].wait()
        for at, weight in ((left, gathered.at[:, 2 * part : 3 * part]), (right, others.at[:, 0:part])):
            out[here, at] = dot(mix_own[here, :], weight[own_rows, :]) + dot(
                mix_other[here, :], weight[other_rows, :]
            )


def local(nx, nz, latents, spectrum, w_value, w_gate, w_out, embed_table, prompt_ids, noise_step):
    rows, chans = latents.shape
    block, part = w_value.shape
    n = nx * nz
    core = lax.axis_index("ch")
    channel = core * part + jnp.arange(part, dtype=jnp.int32)
    emb = step_embedding(noise_step, channel, chans).reshape(1, part)
    half = rows // 2
    groups = nz // STRIDE
    hops = groups - 1
    vmem = pl.BlockSpec(memory_space=pltpu.VMEM)
    dma = pltpu.SemaphoreType.DMA
    exchanged = pltpu.VMEM((n, rows // n, part), BF16)
    plain = pltpu.VMEM((rows, part), BF16)
    summed = pl.pallas_call(
        functools.partial(kernel, nx, nz),
        out_shape=jax.ShapeDtypeStruct((half, chans), F32),
        in_specs=[vmem] * 11,
        out_specs=vmem,
        scratch_shapes=[
            exchanged, exchanged,
            pltpu.VMEM((8, 128), BF16), pltpu.VMEM((half, part), BF16),
            exchanged, exchanged,
            plain, plain, plain,
            pltpu.VMEM((rows, part), F32),
            pltpu.VMEM((nx, groups, STRIDE, block, 3 * part + 128), BF16),
            pltpu.VMEM((nx, groups, STRIDE, block, part + 128), BF16),
            pltpu.VMEM((half, part), BF16), pltpu.VMEM((half, part), BF16),
            pltpu.VMEM((embed_table.shape[1] // 256, 256), F32),
            pltpu.VMEM((rows, rows), BF16), pltpu.VMEM((rows, rows), BF16), pltpu.VMEM((rows, rows), BF16),
            dma((n,)), dma((1,)), dma((n,)), dma((1,)),
            dma((hops,)), dma((hops,)), dma((4, 4)), dma((4, 4)),
            dma((4,)), dma((4,)), dma, dma, dma((2,)), dma((2,)),
        ],
        compiler_params=pltpu.CompilerParams(
            collective_id=0, has_side_effects=True, vmem_limit_bytes=56 * 2**20
        ),
    )(
        latents, spectrum.reshape(rows, part), w_value, w_gate, w_out, embed_table,
        prompt_ids.reshape(1, -1), emb, cas_table(WW), cas_table(HH), cas_table(TT),
    )
    residual = lax.dynamic_slice_in_dim(latents, core * half, half, 0)
    return (residual.astype(F32) + summed).astype(BF16)


def solution(mesh):
    nx, nz = 4, mesh.shape["sp"] // 4
    torus = Mesh(
        mesh.devices.reshape(mesh.shape["grp"], nx, nz, mesh.shape["ch"]),
        ("grp", "sp_0", "sp_1", "ch"),
    )
    in_specs = (
        P(GRP_SP, None),
        P(None, None, SP, "ch"),
        P(SP, "ch"),
        P(SP, "ch"),
        P(SP, None),
        P(SP_CH, None),
        P("grp"),
        P("grp"),
    )
    out_specs = P(GRP_SP_CH, None)
    return jax.shard_map(
        functools.partial(local, nx, nz),
        mesh=torus, in_specs=in_specs, out_specs=out_specs, check_vma=False,
    )
```

```python
import functools
import math

import jax
import jax.numpy as jnp
import numpy as np
from jax import lax
from jax.experimental import pallas as pl
from jax.experimental.pallas import tpu as pltpu
from jax.sharding import Mesh
from jax.sharding import PartitionSpec as P

TT = 16
HH = 64
WW = 128
SP_CH = ("sp_0", "sp_1", "ch")
GRP_SP = ("grp", "sp_0", "sp_1")
GRP_SP_CH = ("grp", "sp_0", "sp_1", "ch")
SP = ("sp_0", "sp_1")
F32 = jnp.float32
BF16 = jnp.bfloat16
MESH = pl.DeviceIdType.MESH
STRIDE = 4
WINDOW = 40


def cas_table(length):
    position = np.arange(length, dtype=np.int32)
    product = position[:, None] * position[None, :] % length
    phase_angle = product.astype(np.float32) * np.float32(2.0 * math.pi / length)
    table = (np.cos(phase_angle) + np.sin(phase_angle)) / np.float32(math.sqrt(length))
    return jnp.asarray(table.astype(jnp.bfloat16))


def step_embedding(noise_step, channel, channels):
    half_count = channels // 2
    lower_half = channel < half_count
    position = jnp.where(lower_half, channel, channel - half_count).astype(jnp.float32)
    frequency = jnp.exp(-math.log(10000.0) * position / half_count)
    phase_angle = noise_step[0].astype(jnp.float32) * frequency
    return jnp.where(lower_half, jnp.sin(phase_angle), jnp.cos(phase_angle))


def dot(a, b):
    return jnp.dot(a, b, preferred_element_type=F32)


def iota(shape, dim):
    return lax.broadcasted_iota(jnp.int32, shape, dim)


def one_hot(condition):
    return jnp.where(condition, 1.0, 0.0).astype(BF16)


def kernel(
    nx, nz,
    lat, spec, wv_in, wg_in, wo_in, table, ids, emb, kw, kh, kt,
    out,
    spread, arrived, spin, spout, back, returned, y_own, y_other, filt, gain, total,
    wall, wo_other, mix_own, mix_other, counts, space, wide, narrow,
    a_send, a_recv, b_send, b_recv, s_send, s_recv, r_send, r_recv,
    y_send, y_recv, o_send, o_recv, m_send, m_recv,
):
    n = nx * nz
    rows, chans = lat.shape
    part = wv_in.shape[1]
    lines = rows // WW
    block = rows // n
    mx, mz, core = lax.axis_index("sp_0"), lax.axis_index("sp_1"), lax.axis_index("ch")
    me = mx * nz + mz
    other_core = {"ch": 1 - core}
    tile = rows // nx
    per = tile // block

    def x_step(turn):
        return jnp.where(turn == 0, 2, jnp.where(turn == 1, 1, jnp.where(turn == 2, 3, 0)))

    def partner(i):
        zi = nz - 1 - i % nz
        m = (zi + 1) // 2
        dz = jnp.where(zi % 2 == 1, m, nz - m) % nz
        tx, tz = (mx + x_step(i // nz)) % nx, (mz + dz) % nz
        return {"sp_0": tx, "sp_1": tz}, tx * nz + tz

    def blocks_of(column):
        return pl.ds(pl.multiple_of(column * nz, nz), nz)

    def rows_of(column):
        return pl.ds(pl.multiple_of(column * tile, tile), tile)

    barrier = pltpu.get_barrier_semaphore()

    def greet(i, carry):
        device, _ = partner(i)
        pl.semaphore_signal(barrier, inc=1, device_id=device, device_id_type=MESH)
        return carry

    lax.fori_loop(0, n - 1, greet, 0)
    pl.semaphore_signal(barrier, inc=1, device_id=other_core, device_id_type=MESH)

    pick = one_hot(iota((rows, WW), 0) // lines == iota((rows, WW), 1))
    spread_rows = dot(pick, kw[...]).astype(BF16)
    line_of = iota((rows, WW), 0) % lines
    for line in range(lines):
        narrow[:, line * WW : (line + 1) * WW] = jnp.where(
            line_of == line, spread_rows, jnp.zeros_like(spread_rows)
        )
    mine = pl.ds(pl.multiple_of(core * part, 128), part)

    def widen(r, carry):
        at = pl.ds(pl.multiple_of(r * tile, tile), tile)
        got = dot(narrow[at, :], lat[:, mine]).astype(BF16)
        spread[pl.ds(r * per, per)] = got.reshape(per, block, part)
        return carry

    lax.fori_loop(0, rows // tile, widen, 0)
    arrived[me] = spread[me]
    wall[mx, mz // STRIDE, mz % STRIDE, :, 0:part] = wv_in[...]
    wall[mx, mz // STRIDE, mz % STRIDE, :, part : 2 * part] = wg_in[...]
    wall[mx, mz // STRIDE, mz % STRIDE, :, 2 * part : 3 * part] = wo_in[:, mine]

    pl.semaphore_wait(barrier, n)

    groups = nz // STRIDE
    up = (groups + 1) // 2
    down = groups - 1 - up

    first_part = pl.ds(0, part)
    later_part = pl.ds(part, 2 * part + 128)

    def hop(direction, q):
        origin = (mz // STRIDE - direction * (q - 1) + groups) % groups
        ref = wall.at[mx, origin, mz % STRIDE]
        k = (q - 1) if direction > 0 else up + q - 1
        return pltpu.make_async_remote_copy(
            src_ref=ref, dst_ref=ref, send_sem=s_send.at[k], recv_sem=s_recv.at[k],
            device_id={"sp_1": (mz + direction * STRIDE + nz) % nz}, device_id_type=MESH,
        )

    def hop_in(q):
        hop(1, q).wait_recv()
        if q <= down:
            hop(-1, q).wait_recv()

    def hop_out(q):
        hop(1, q).start()
        if q <= down:
            hop(-1, q).start()

    def group_span(k):
        return ((0, groups), (0, groups), (groups // 2, groups), (0, groups // 2))[k]

    def piece(stage, k, g, count):
        step = (1, -1, 1, -1)[k]
        back_by = (0, 0, 1, -1)[k]
        lanes = (first_part, later_part)[stage // 2]
        if stage % 2:
            ref = wall.at[(mx - back_by + nx) % nx, pl.ds(g, count), :, :, lanes]
            device = {"sp_0": (mx + step + nx) % nx}
        else:
            ref = wall.at[mx, pl.ds(g, count), (mz - back_by + nz) % STRIDE, :, lanes]
            device = {"sp_1": (mz + step + nz) % nz}
        return pltpu.make_async_remote_copy(
            src_ref=ref, dst_ref=ref, send_sem=r_send.at[stage, k], recv_sem=r_recv.at[stage, k],
            device_id=device, device_id_type=MESH,
        )

    def whole(stage, k):
        low, high = group_span(k)
        return piece(stage, k, low, high - low)

    def exchange(src, dst, send_sem, recv_sem):
        def copy(i):
            device, target = partner(i)
            return pltpu.make_async_remote_copy(
                src_ref=src.at[target], dst_ref=dst.at[me],
                send_sem=send_sem.at[i], recv_sem=recv_sem.at[i // nz],
                device_id=device, device_id_type=MESH,
            )

        def send(first, last):
            def body(i, carry):
                @pl.when(i >= WINDOW)
                def _():
                    copy(i - WINDOW).wait_send()

                copy(i).start()
                return carry

            lax.fori_loop(first, last, body, 0)

        def drain():
            def body(i, carry):
                copy(i).wait_send()
                return carry

            lax.fori_loop(n - 1 - WINDOW, n - 1, body, 0)

        def arrive(turn):
            column = (mx - (2, 1, 3, 0)[turn] + nx) % nx
            some = dst.at[pl.ds(column * nz, nz - 1 if turn == nx - 1 else nz)]
            pltpu.make_async_copy(some, some, recv_sem.at[turn]).wait()
            return column

        return send, drain, arrive

    send, drain, arrive = exchange(spread, arrived, a_send, a_recv)
    send(0, 8)

    vocab = table.shape[1]
    low_count = 256
    high_count = vocab // low_count
    prompt = ids.shape[1]
    high_hot = one_hot(ids[...] // low_count == iota((high_count, prompt), 0))
    low_hot = one_hot(ids[...] % low_count == iota((low_count, prompt), 0))
    counts[...] = lax.dot_general(
        high_hot, low_hot, (((1,), (1,)), ((), ())), preferred_element_type=F32
    )

    def tally(h, total):
        piece = table[:, pl.ds(pl.multiple_of(h * low_count, low_count), low_count)]
        return total + piece.astype(F32) * counts[pl.ds(h, 1), :]

    few = table.shape[0]
    tallied = lax.fori_loop(0, high_count, tally, jnp.zeros((few, low_count), F32))
    pooled4 = jnp.sum(tallied, axis=1, keepdims=True) * (1.0 / prompt)
    pooled8 = jnp.concatenate([pooled4] * (block // few), axis=0)
    pooled8 = jnp.where(iota((block, 1), 0) // few == core, pooled8, 0.0)
    first = pooled8.astype(BF16).astype(F32)
    second = (pooled8 - first).astype(BF16).astype(F32)
    third = pooled8 - first - second
    lane = iota((block, 128), 1)
    terms = jnp.where(lane == 0, first, jnp.where(lane == 1, second, jnp.where(lane == 2, third, 0.0)))
    wall[mx, mz // STRIDE, mz % STRIDE, :, 3 * part : 3 * part + 128] = terms.astype(BF16)
    hop_out(1)

    def send_hops(at, pace):
        for q in range(1, up + 1):
            send(at, at + pace)
            at += pace
            hop_in(q)
            if q < up:
                hop_out(q + 1)
        return at

    def send_pieces(stage, at, each, slack):
        for pair in ((0, 1), (2, 3)):
            count = group_span(pair[0])[1] - group_span(pair[0])[0]

            def body(g, carry, at=at, pair=pair):
                for k in pair:
                    piece(stage, k, group_span(k)[0] + g, 1).start()
                send(at + g * each, at + (g + 1) * each)
                return carry

            lax.fori_loop(0, count, body, 0)
            at += count * each
            send(at, at + slack)
            at += slack
            for k in pair:
                whole(stage, k).wait_recv()
        return at

    cells = TT * HH
    kt_wide = dot(kt[...], one_hot(iota((TT, cells), 1) // HH == iota((TT, cells), 0)))
    kh_wide = dot(kh[...], one_hot(iota((HH, cells), 1) % HH == iota((HH, cells), 0)))
    for s in range(TT):
        space[s * HH : (s + 1) * HH, :] = (kh_wide * kt_wide[s : s + 1, :]).astype(BF16)
    kw_wide = dot(kw[...], one_hot(iota((WW, rows), 1) // lines == iota((WW, rows), 0)))
    column_line = iota((WW, rows), 1) % lines
    for line in range(lines):
        wide[line * WW : (line + 1) * WW, :] = jnp.where(column_line == line, kw_wide, 0.0).astype(BF16)
    at = send_hops(8, 13)
    at = send_pieces(0, at, 1, 8)
    at = send_pieces(1, at, 1, 8)
    send(at, n - 1)
    for turn in range(nx - 1):
        column = arrive(turn)
        for r in range(nx):
            here = slice(r * tile, (r + 1) * tile)
            got = dot(space[here, rows_of(column)], arrived[blocks_of(column)].reshape(tile, part))
            total[here, :] = got if turn == 0 else total[here, :] + got
    drain()
    column = arrive(nx - 1)

    quarters = rows // tile
    gathered = wall.reshape(chans, 3 * part + 128)
    value_weight = gathered.at[:, 0:part]
    own_rows = pl.ds(pl.multiple_of(core * part, part), part)
    other_rows = pl.ds(pl.multiple_of((1 - core) * part, part), part)
    ycopies = [
        pltpu.make_async_remote_copy(
            src_ref=y_own.at[pl.ds(r * tile, tile)], dst_ref=y_other.at[pl.ds(r * tile, tile)],
            send_sem=y_send.at[r], recv_sem=y_recv.at[r], device_id=other_core, device_id_type=MESH,
        )
        for r in range(quarters)
    ]

    def forward(r):
        here = slice(r * tile, (r + 1) * tile)
        got = dot(space[here, rows_of(column)], arrived[blocks_of(column)].reshape(tile, part))
        y_own[here, :] = (total[here, :] + got).astype(BF16)
        ycopies[r].start()

    def project(r):
        here = slice(r * tile, (r + 1) * tile)
        ycopies[r].wait_recv()
        value = dot(y_own[here, :], value_weight[own_rows, :])
        value = value + dot(y_other[here, :], value_weight[other_rows, :])
        filt[here, :] = (value * spec[here, :].astype(F32)).astype(BF16)

    def backward(turn):
        target = (mx + (2, 1, 3, 0)[turn]) % nx
        got = dot(space[rows_of(target), :], filt[...]).astype(BF16)
        back[blocks_of(target)] = got.reshape(per, block, part)

    whole(2, 0).start()
    whole(2, 1).start()
    for r in range(nx):
        forward(r)
    for r in range(nx):
        project(r)
    whole(2, 0).wait_recv()
    whole(2, 1).wait_recv()
    whole(2, 2).start()
    whole(2, 3).start()
    send, drain, arrive = exchange(back, returned, b_send, b_recv)
    backward(0)
    send(0, nz // 2)
    backward(1)
    send(nz // 2, nz)
    for turn in range(2, nx):
        backward(turn)
    returned[me] = back[me]
    for r in range(nx):
        ycopies[r].wait_send()
    whole(2, 2).wait_recv()
    whole(2, 3).wait_recv()
    at = send_pieces(3, nz, 4, 16)
    send(at, n - 1)
    for q in range(1, up + 1):
        hop(1, q).wait_send()
        if q <= down:
            hop(-1, q).wait_send()
    for stage in range(4):
        for k in range(4):
            whole(stage, k).wait_send()

    upper = pl.ds(2 * part, part + 128)
    swap_out = pltpu.make_async_remote_copy(
        src_ref=wall.at[:, :, :, :, upper], dst_ref=wo_other, send_sem=o_send, recv_sem=o_recv,
        device_id=other_core, device_id_type=MESH,
    )
    swap_out.start()
    swap_out.wait()
    others = wo_other.reshape(chans, part + 128)
    pools = gathered[:, 3 * part : 3 * part + 128] + others[:, part : part + 128]
    chosen = one_hot(iota((chans, part), 0) == iota((chans, part), 1) + core * part)
    terms = lax.dot_general(pools, chosen, (((0,), (0,)), ((), ())), preferred_element_type=F32)
    modulation = 1.0 + jnp.sum(terms[0:8, :], axis=0, keepdims=True) + emb[...]

    def gate(r, carry):
        here = pl.ds(pl.multiple_of(r * tile, tile), tile)
        v = dot(lat[here, :], gathered[:, part : 2 * part])
        gain[here, :] = v / (1.0 + jnp.exp(-v)) * modulation
        return carry

    lax.fori_loop(0, quarters, gate, 0)
    for turn in range(nx - 1):
        column = arrive(turn)
        for r in range(nx):
            here = slice(r * tile, (r + 1) * tile)
            got = dot(wide[here, rows_of(column)], returned[blocks_of(column)].reshape(tile, part))
            total[here, :] = got if turn == 0 else total[here, :] + got
    drain()
    last = arrive(nx - 1)

    half = rows // 2

    def finish(r, dst, base):
        here = pl.ds(pl.multiple_of(base + r * tile, tile), tile)
        mix = dot(wide[here, rows_of(last)], returned[blocks_of(last)].reshape(tile, part))
        mix = (total[here, :] + mix) * gain[here, :]
        dst[pl.ds(pl.multiple_of(r * tile, tile), tile), :] = mix.astype(BF16)

    mcopies = []
    for r in range(half // tile):
        finish(r, spout, (1 - core) * half)
        mcopies.append(pltpu.make_async_remote_copy(
            src_ref=spout.at[pl.ds(r * tile, tile)], dst_ref=mix_other.at[pl.ds(r * tile, tile)],
            send_sem=m_send.at[r], recv_sem=m_recv.at[r], device_id=other_core, device_id_type=MESH,
        ))
        mcopies[-1].start()
    for r in range(half // tile):
        finish(r, mix_own, core * half)
    left = pl.ds(pl.multiple_of(core * part, part), part)
    right = pl.ds(pl.multiple_of((1 - core) * part, part), part)
    for r in range(half // tile):
        here = slice(r * tile, (r + 1) * tile)
        mcopies[r].wait()
        for at, weight in ((left, gathered.at[:, 2 * part : 3 * part]), (right, others.at[:, 0:part])):
            out[here, at] = dot(mix_own[here, :], weight[own_rows, :]) + dot(
                mix_other[here, :], weight[other_rows, :]
            )


def local(nx, nz, latents, spectrum, w_value, w_gate, w_out, embed_table, prompt_ids, noise_step):
    rows, chans = latents.shape
    block, part = w_value.shape
    n = nx * nz
    core = lax.axis_index("ch")
    channel = core * part + jnp.arange(part, dtype=jnp.int32)
    emb = step_embedding(noise_step, channel, chans).reshape(1, part)
    half = rows // 2
    groups = nz // STRIDE
    hops = groups - 1
    vmem = pl.BlockSpec(memory_space=pltpu.VMEM)
    dma = pltpu.SemaphoreType.DMA
    exchanged = pltpu.VMEM((n, rows // n, part), BF16)
    plain = pltpu.VMEM((rows, part), BF16)
    summed = pl.pallas_call(
        functools.partial(kernel, nx, nz),
        out_shape=jax.ShapeDtypeStruct((half, chans), F32),
        in_specs=[vmem] * 11,
        out_specs=vmem,
        scratch_shapes=[
            exchanged, exchanged,
            pltpu.VMEM((8, 128), BF16), pltpu.VMEM((half, part), BF16),
            exchanged, exchanged,
            plain, plain, plain,
            pltpu.VMEM((rows, part), F32), pltpu.VMEM((rows, part), F32),
            pltpu.VMEM((nx, groups, STRIDE, block, 3 * part + 128), BF16),
            pltpu.VMEM((nx, groups, STRIDE, block, part + 128), BF16),
            pltpu.VMEM((half, part), BF16), pltpu.VMEM((half, part), BF16),
            pltpu.VMEM((embed_table.shape[1] // 256, 256), F32),
            pltpu.VMEM((rows, rows), BF16), pltpu.VMEM((rows, rows), BF16), pltpu.VMEM((rows, rows), BF16),
            dma((n,)), dma((nx,)), dma((n,)), dma((nx,)),
            dma((hops,)), dma((hops,)), dma((4, 4)), dma((4, 4)),
            dma((4,)), dma((4,)), dma, dma, dma((2,)), dma((2,)),
        ],
        compiler_params=pltpu.CompilerParams(
            collective_id=0, has_side_effects=True, vmem_limit_bytes=56 * 2**20
        ),
    )(
        latents, spectrum.reshape(rows, part), w_value, w_gate, w_out, embed_table,
        prompt_ids.reshape(1, -1), emb, cas_table(WW), cas_table(HH), cas_table(TT),
    )
    residual = lax.dynamic_slice_in_dim(latents, core * half, half, 0)
    return (residual.astype(F32) + summed).astype(BF16)


def solution(mesh):
    nx, nz = 4, mesh.shape["sp"] // 4
    torus = Mesh(
        mesh.devices.reshape(mesh.shape["grp"], nx, nz, mesh.shape["ch"]),
        ("grp", "sp_0", "sp_1", "ch"),
    )
    in_specs = (
        P(GRP_SP, None),
        P(None, None, SP, "ch"),
        P(SP, "ch"),
        P(SP, "ch"),
        P(SP, None),
        P(SP_CH, None),
        P("grp"),
        P("grp"),
    )
    out_specs = P(GRP_SP_CH, None)
    return jax.shard_map(
        functools.partial(local, nx, nz),
        mesh=torus, in_specs=in_specs, out_specs=out_specs, check_vma=False,
    )
```

```python
import functools
import math

import jax
import jax.numpy as jnp
import numpy as np
from jax import lax
from jax.experimental import pallas as pl
from jax.experimental.pallas import tpu as pltpu
from jax.sharding import Mesh
from jax.sharding import PartitionSpec as P

TT = 16
HH = 64
WW = 128
SP_CH = ("sp_0", "sp_1", "ch")
GRP_SP = ("grp", "sp_0", "sp_1")
GRP_SP_CH = ("grp", "sp_0", "sp_1", "ch")
SP = ("sp_0", "sp_1")
F32 = jnp.float32
BF16 = jnp.bfloat16
MESH = pl.DeviceIdType.MESH
STRIDE = 4
WINDOW = 64


def cas_table(length):
    position = np.arange(length, dtype=np.int32)
    product = position[:, None] * position[None, :] % length
    phase_angle = product.astype(np.float32) * np.float32(2.0 * math.pi / length)
    table = (np.cos(phase_angle) + np.sin(phase_angle)) / np.float32(math.sqrt(length))
    return jnp.asarray(table.astype(jnp.bfloat16))


def step_embedding(noise_step, channel, channels):
    half_count = channels // 2
    lower_half = channel < half_count
    position = jnp.where(lower_half, channel, channel - half_count).astype(jnp.float32)
    frequency = jnp.exp(-math.log(10000.0) * position / half_count)
    phase_angle = noise_step[0].astype(jnp.float32) * frequency
    return jnp.where(lower_half, jnp.sin(phase_angle), jnp.cos(phase_angle))


def dot(a, b):
    return jnp.dot(a, b, preferred_element_type=F32)


def iota(shape, dim):
    return lax.broadcasted_iota(jnp.int32, shape, dim)


def one_hot(condition):
    return jnp.where(condition, 1.0, 0.0).astype(BF16)


def kernel(
    nx, nz,
    lat, spec, wv_in, wg_in, wo_in, table, ids, emb, kw, kh, kt,
    out,
    spread, arrived, spin, spout, back, returned, y_own, y_other, filt, gain, total,
    wall, wo_other, mix_own, mix_other, counts, space, wide, narrow,
    a_send, a_recv, b_send, b_recv, s_send, s_recv, r_send, r_recv,
    y_send, y_recv, o_send, o_recv, m_send, m_recv,
):
    n = nx * nz
    rows, chans = lat.shape
    part = wv_in.shape[1]
    lines = rows // WW
    block = rows // n
    mx, mz, core = lax.axis_index("sp_0"), lax.axis_index("sp_1"), lax.axis_index("ch")
    me = mx * nz + mz
    other_core = {"ch": 1 - core}
    tile = rows // nx
    per = tile // block

    def x_step(turn):
        return jnp.where(turn == 0, 2, jnp.where(turn == 1, 1, jnp.where(turn == 2, 3, 0)))

    def partner(i):
        zi = nz - 1 - i % nz
        m = (zi + 1) // 2
        dz = jnp.where(zi % 2 == 1, m, nz - m) % nz
        tx, tz = (mx + x_step(i // nz)) % nx, (mz + dz) % nz
        return {"sp_0": tx, "sp_1": tz}, tx * nz + tz

    def blocks_of(column):
        return pl.ds(pl.multiple_of(column * nz, nz), nz)

    def rows_of(column):
        return pl.ds(pl.multiple_of(column * tile, tile), tile)

    barrier = pltpu.get_barrier_semaphore()

    def greet(i, carry):
        device, _ = partner(i)
        pl.semaphore_signal(barrier, inc=1, device_id=device, device_id_type=MESH)
        return carry

    lax.fori_loop(0, n - 1, greet, 0)
    pl.semaphore_signal(barrier, inc=1, device_id=other_core, device_id_type=MESH)

    pick = one_hot(iota((rows, WW), 0) // lines == iota((rows, WW), 1))
    spread_rows = dot(pick, kw[...]).astype(BF16)
    line_of = iota((rows, WW), 0) % lines
    for line in range(lines):
        narrow[:, line * WW : (line + 1) * WW] = jnp.where(
            line_of == line, spread_rows, jnp.zeros_like(spread_rows)
        )
    mine = pl.ds(pl.multiple_of(core * part, 128), part)

    def widen(r, carry):
        at = pl.ds(pl.multiple_of(r * tile, tile), tile)
        got = dot(narrow[at, :], lat[:, mine]).astype(BF16)
        spread[pl.ds(r * per, per)] = got.reshape(per, block, part)
        return carry

    lax.fori_loop(0, rows // tile, widen, 0)
    arrived[me] = spread[me]
    wall[mx, mz // STRIDE, mz % STRIDE, :, 0:part] = wv_in[...]
    wall[mx, mz // STRIDE, mz % STRIDE, :, part : 2 * part] = wg_in[...]
    wall[mx, mz // STRIDE, mz % STRIDE, :, 2 * part : 3 * part] = wo_in[:, mine]

    pl.semaphore_wait(barrier, n)

    groups = nz // STRIDE
    up = (groups + 1) // 2
    down = groups - 1 - up

    first_part = pl.ds(0, part)
    later_part = pl.ds(part, 2 * part + 128)

    def hop(direction, q):
        origin = (mz // STRIDE - direction * (q - 1) + groups) % groups
        ref = wall.at[mx, origin, mz % STRIDE]
        k = (q - 1) if direction > 0 else up + q - 1
        return pltpu.make_async_remote_copy(
            src_ref=ref, dst_ref=ref, send_sem=s_send.at[k], recv_sem=s_recv.at[k],
            device_id={"sp_1": (mz + direction * STRIDE + nz) % nz}, device_id_type=MESH,
        )

    def hop_in(q):
        hop(1, q).wait_recv()
        if q <= down:
            hop(-1, q).wait_recv()

    def hop_out(q):
        hop(1, q).start()
        if q <= down:
            hop(-1, q).start()

    def group_span(k):
        return ((0, groups), (0, groups), (groups // 2, groups), (0, groups // 2))[k]

    def piece(stage, k, g, count):
        step = (1, -1, 1, -1)[k]
        back_by = (0, 0, 1, -1)[k]
        lanes = (first_part, later_part)[stage // 2]
        if stage % 2:
            ref = wall.at[(mx - back_by + nx) % nx, pl.ds(g, count), :, :, lanes]
            device = {"sp_0": (mx + step + nx) % nx}
        else:
            ref = wall.at[mx, pl.ds(g, count), (mz - back_by + nz) % STRIDE, :, lanes]
            device = {"sp_1": (mz + step + nz) % nz}
        return pltpu.make_async_remote_copy(
            src_ref=ref, dst_ref=ref, send_sem=r_send.at[stage, k], recv_sem=r_recv.at[stage, k],
            device_id=device, device_id_type=MESH,
        )

    def whole(stage, k):
        low, high = group_span(k)
        return piece(stage, k, low, high - low)

    def exchange(src, dst, send_sem, recv_sem):
        def copy(i):
            device, target = partner(i)
            return pltpu.make_async_remote_copy(
                src_ref=src.at[target], dst_ref=dst.at[me],
                send_sem=send_sem.at[i], recv_sem=recv_sem.at[i // nz],
                device_id=device, device_id_type=MESH,
            )

        def send(first, last):
            def body(i, carry):
                @pl.when(i >= WINDOW)
                def _():
                    copy(i - WINDOW).wait_send()

                copy(i).start()
                return carry

            lax.fori_loop(first, last, body, 0)

        def drain():
            def body(i, carry):
                copy(i).wait_send()
                return carry

            lax.fori_loop(n - 1 - WINDOW, n - 1, body, 0)

        def arrive(turn):
            column = (mx - (2, 1, 3, 0)[turn] + nx) % nx
            some = dst.at[pl.ds(column * nz, nz - 1 if turn == nx - 1 else nz)]
            pltpu.make_async_copy(some, some, recv_sem.at[turn]).wait()
            return column

        return send, drain, arrive

    send, drain, arrive = exchange(spread, arrived, a_send, a_recv)
    send(0, 8)

    vocab = table.shape[1]
    low_count = 256
    high_count = vocab // low_count
    prompt = ids.shape[1]
    high_hot = one_hot(ids[...] // low_count == iota((high_count, prompt), 0))
    low_hot = one_hot(ids[...] % low_count == iota((low_count, prompt), 0))
    counts[...] = lax.dot_general(
        high_hot, low_hot, (((1,), (1,)), ((), ())), preferred_element_type=F32
    )

    def tally(h, total):
        piece = table[:, pl.ds(pl.multiple_of(h * low_count, low_count), low_count)]
        return total + piece.astype(F32) * counts[pl.ds(h, 1), :]

    few = table.shape[0]
    tallied = lax.fori_loop(0, high_count, tally, jnp.zeros((few, low_count), F32))
    pooled4 = jnp.sum(tallied, axis=1, keepdims=True) * (1.0 / prompt)
    pooled8 = jnp.concatenate([pooled4] * (block // few), axis=0)
    pooled8 = jnp.where(iota((block, 1), 0) // few == core, pooled8, 0.0)
    first = pooled8.astype(BF16).astype(F32)
    second = (pooled8 - first).astype(BF16).astype(F32)
    third = pooled8 - first - second
    lane = iota((block, 128), 1)
    terms = jnp.where(lane == 0, first, jnp.where(lane == 1, second, jnp.where(lane == 2, third, 0.0)))
    wall[mx, mz // STRIDE, mz % STRIDE, :, 3 * part : 3 * part + 128] = terms.astype(BF16)
    hop_out(1)

    def send_hops(at, pace):
        for q in range(1, up + 1):
            send(at, at + pace)
            at += pace
            hop_in(q)
            if q < up:
                hop_out(q + 1)
        return at

    def send_pieces(stage, at, each, slack):
        for pair in ((0, 1), (2, 3)):
            count = group_span(pair[0])[1] - group_span(pair[0])[0]

            def body(g, carry, at=at, pair=pair):
                for k in pair:
                    piece(stage, k, group_span(k)[0] + g, 1).start()
                send(at + g * each, at + (g + 1) * each)
                return carry

            lax.fori_loop(0, count, body, 0)
            at += count * each
            send(at, at + slack)
            at += slack
            for k in pair:
                whole(stage, k).wait_recv()
        return at

    cells = TT * HH
    kt_wide = dot(kt[...], one_hot(iota((TT, cells), 1) // HH == iota((TT, cells), 0)))
    kh_wide = dot(kh[...], one_hot(iota((HH, cells), 1) % HH == iota((HH, cells), 0)))
    for s in range(TT):
        space[s * HH : (s + 1) * HH, :] = (kh_wide * kt_wide[s : s + 1, :]).astype(BF16)
    kw_wide = dot(kw[...], one_hot(iota((WW, rows), 1) // lines == iota((WW, rows), 0)))
    column_line = iota((WW, rows), 1) % lines
    for line in range(lines):
        wide[line * WW : (line + 1) * WW, :] = jnp.where(column_line == line, kw_wide, 0.0).astype(BF16)
    at = send_hops(8, 13)
    at = send_pieces(0, at, 1, 8)
    at = send_pieces(1, at, 1, 8)
    send(at, n - 1)
    for turn in range(nx - 1):
        column = arrive(turn)
        for r in range(nx):
            here = slice(r * tile, (r + 1) * tile)
            got = dot(space[here, rows_of(column)], arrived[blocks_of(column)].reshape(tile, part))
            total[here, :] = got if turn == 0 else total[here, :] + got
    drain()
    column = arrive(nx - 1)

    quarters = rows // tile
    gathered = wall.reshape(chans, 3 * part + 128)
    value_weight = gathered.at[:, 0:part]
    own_rows = pl.ds(pl.multiple_of(core * part, part), part)
    other_rows = pl.ds(pl.multiple_of((1 - core) * part, part), part)
    ycopies = [
        pltpu.make_async_remote_copy(
            src_ref=y_own.at[pl.ds(r * tile, tile)], dst_ref=y_other.at[pl.ds(r * tile, tile)],
            send_sem=y_send.at[r], recv_sem=y_recv.at[r], device_id=other_core, device_id_type=MESH,
        )
        for r in range(quarters)
    ]

    def forward(r):
        here = slice(r * tile, (r + 1) * tile)
        got = dot(space[here, rows_of(column)], arrived[blocks_of(column)].reshape(tile, part))
        y_own[here, :] = (total[here, :] + got).astype(BF16)
        ycopies[r].start()

    def project(r):
        here = slice(r * tile, (r + 1) * tile)
        ycopies[r].wait_recv()
        value = dot(y_own[here, :], value_weight[own_rows, :])
        value = value + dot(y_other[here, :], value_weight[other_rows, :])
        filt[here, :] = (value * spec[here, :].astype(F32)).astype(BF16)

    def backward(turn):
        target = (mx + (2, 1, 3, 0)[turn]) % nx
        got = dot(space[rows_of(target), :], filt[...]).astype(BF16)
        back[blocks_of(target)] = got.reshape(per, block, part)

    whole(2, 0).start()
    whole(2, 1).start()
    for r in range(nx):
        forward(r)
    for r in range(nx):
        project(r)
    whole(2, 0).wait_recv()
    whole(2, 1).wait_recv()
    whole(2, 2).start()
    whole(2, 3).start()
    send, drain, arrive = exchange(back, returned, b_send, b_recv)
    backward(0)
    send(0, nz // 2)
    backward(1)
    send(nz // 2, nz)
    for turn in range(2, nx):
        backward(turn)
    returned[me] = back[me]
    for r in range(nx):
        ycopies[r].wait_send()
    whole(2, 2).wait_recv()
    whole(2, 3).wait_recv()
    at = send_pieces(3, nz, 4, 16)
    send(at, n - 1)
    for q in range(1, up + 1):
        hop(1, q).wait_send()
        if q <= down:
            hop(-1, q).wait_send()
    for stage in range(4):
        for k in range(4):
            whole(stage, k).wait_send()

    upper = pl.ds(2 * part, part + 128)
    swap_out = pltpu.make_async_remote_copy(
        src_ref=wall.at[:, :, :, :, upper], dst_ref=wo_other, send_sem=o_send, recv_sem=o_recv,
        device_id=other_core, device_id_type=MESH,
    )
    swap_out.start()
    swap_out.wait()
    others = wo_other.reshape(chans, part + 128)
    pools = gathered[:, 3 * part : 3 * part + 128] + others[:, part : part + 128]
    chosen = one_hot(iota((chans, part), 0) == iota((chans, part), 1) + core * part)
    terms = lax.dot_general(pools, chosen, (((0,), (0,)), ((), ())), preferred_element_type=F32)
    modulation = 1.0 + jnp.sum(terms[0:8, :], axis=0, keepdims=True) + emb[...]

    def gate(r, carry):
        here = pl.ds(pl.multiple_of(r * tile, tile), tile)
        v = dot(lat[here, :], gathered[:, part : 2 * part])
        gain[here, :] = v / (1.0 + jnp.exp(-v)) * modulation
        return carry

    lax.fori_loop(0, quarters, gate, 0)
    for turn in range(nx - 1):
        column = arrive(turn)
        for r in range(nx):
            here = slice(r * tile, (r + 1) * tile)
            got = dot(wide[here, rows_of(column)], returned[blocks_of(column)].reshape(tile, part))
            total[here, :] = got if turn == 0 else total[here, :] + got
    drain()
    last = arrive(nx - 1)

    half = rows // 2

    def finish(r, dst, base):
        here = pl.ds(pl.multiple_of(base + r * tile, tile), tile)
        mix = dot(wide[here, rows_of(last)], returned[blocks_of(last)].reshape(tile, part))
        mix = (total[here, :] + mix) * gain[here, :]
        dst[pl.ds(pl.multiple_of(r * tile, tile), tile), :] = mix.astype(BF16)

    mcopies = []
    for r in range(half // tile):
        finish(r, spout, (1 - core) * half)
        mcopies.append(pltpu.make_async_remote_copy(
            src_ref=spout.at[pl.ds(r * tile, tile)], dst_ref=mix_other.at[pl.ds(r * tile, tile)],
            send_sem=m_send.at[r], recv_sem=m_recv.at[r], device_id=other_core, device_id_type=MESH,
        ))
        mcopies[-1].start()
    for r in range(half // tile):
        finish(r, mix_own, core * half)
    left = pl.ds(pl.multiple_of(core * part, part), part)
    right = pl.ds(pl.multiple_of((1 - core) * part, part), part)
    for r in range(half // tile):
        here = slice(r * tile, (r + 1) * tile)
        mcopies[r].wait()
        own_cells = pl.ds(pl.multiple_of(core * half + r * tile, tile), tile)
        for at, weight in ((left, gathered.at[:, 2 * part : 3 * part]), (right, others.at[:, 0:part])):
            added = dot(mix_own[here, :], weight[own_rows, :]) + dot(
                mix_other[here, :], weight[other_rows, :]
            )
            out[here, at] = (lat[own_cells, at].astype(F32) + added).astype(BF16)


def local(nx, nz, latents, spectrum, w_value, w_gate, w_out, embed_table, prompt_ids, noise_step):
    rows, chans = latents.shape
    block, part = w_value.shape
    n = nx * nz
    core = lax.axis_index("ch")
    channel = core * part + jnp.arange(part, dtype=jnp.int32)
    emb = step_embedding(noise_step, channel, chans).reshape(1, part)
    half = rows // 2
    groups = nz // STRIDE
    hops = groups - 1
    vmem = pl.BlockSpec(memory_space=pltpu.VMEM)
    dma = pltpu.SemaphoreType.DMA
    exchanged = pltpu.VMEM((n, rows // n, part), BF16)
    plain = pltpu.VMEM((rows, part), BF16)
    return pl.pallas_call(
        functools.partial(kernel, nx, nz),
        out_shape=jax.ShapeDtypeStruct((half, chans), BF16),
        in_specs=[vmem] * 11,
        out_specs=vmem,
        scratch_shapes=[
            exchanged, exchanged,
            pltpu.VMEM((8, 128), BF16), pltpu.VMEM((half, part), BF16),
            exchanged, exchanged,
            plain, plain, plain,
            pltpu.VMEM((rows, part), F32), pltpu.VMEM((rows, part), F32),
            pltpu.VMEM((nx, groups, STRIDE, block, 3 * part + 128), BF16),
            pltpu.VMEM((nx, groups, STRIDE, block, part + 128), BF16),
            pltpu.VMEM((half, part), BF16), pltpu.VMEM((half, part), BF16),
            pltpu.VMEM((embed_table.shape[1] // 256, 256), F32),
            pltpu.VMEM((rows, rows), BF16), pltpu.VMEM((rows, rows), BF16), pltpu.VMEM((rows, rows), BF16),
            dma((n,)), dma((nx,)), dma((n,)), dma((nx,)),
            dma((hops,)), dma((hops,)), dma((4, 4)), dma((4, 4)),
            dma((4,)), dma((4,)), dma, dma, dma((2,)), dma((2,)),
        ],
        compiler_params=pltpu.CompilerParams(
            collective_id=0, has_side_effects=True, vmem_limit_bytes=56 * 2**20
        ),
    )(
        latents, spectrum.reshape(rows, part), w_value, w_gate, w_out, embed_table,
        prompt_ids.reshape(1, -1), emb, cas_table(WW), cas_table(HH), cas_table(TT),
    )


def solution(mesh):
    nx, nz = 4, mesh.shape["sp"] // 4
    torus = Mesh(
        mesh.devices.reshape(mesh.shape["grp"], nx, nz, mesh.shape["ch"]),
        ("grp", "sp_0", "sp_1", "ch"),
    )
    in_specs = (
        P(GRP_SP, None),
        P(None, None, SP, "ch"),
        P(SP, "ch"),
        P(SP, "ch"),
        P(SP, None),
        P(SP_CH, None),
        P("grp"),
        P("grp"),
    )
    out_specs = P(GRP_SP_CH, None)
    return jax.shard_map(
        functools.partial(local, nx, nz),
        mesh=torus, in_specs=in_specs, out_specs=out_specs, check_vma=False,
    )
```

```python
import functools
import math

import jax
import jax.numpy as jnp
import numpy as np
from jax import lax
from jax.experimental import pallas as pl
from jax.experimental.pallas import tpu as pltpu
from jax.sharding import Mesh
from jax.sharding import PartitionSpec as P

TT = 16
HH = 64
WW = 128
SP_CH = ("sp_0", "sp_1", "ch")
GRP_SP = ("grp", "sp_0", "sp_1")
GRP_SP_CH = ("grp", "sp_0", "sp_1", "ch")
SP = ("sp_0", "sp_1")
F32 = jnp.float32
BF16 = jnp.bfloat16
MESH = pl.DeviceIdType.MESH
STRIDE = 4
WINDOW = 96


def cas_table(length):
    position = np.arange(length, dtype=np.int32)
    product = position[:, None] * position[None, :] % length
    phase_angle = product.astype(np.float32) * np.float32(2.0 * math.pi / length)
    table = (np.cos(phase_angle) + np.sin(phase_angle)) / np.float32(math.sqrt(length))
    return jnp.asarray(table.astype(jnp.bfloat16))


def step_embedding(noise_step, channel, channels):
    half_count = channels // 2
    lower_half = channel < half_count
    position = jnp.where(lower_half, channel, channel - half_count).astype(jnp.float32)
    frequency = jnp.exp(-math.log(10000.0) * position / half_count)
    phase_angle = noise_step[0].astype(jnp.float32) * frequency
    return jnp.where(lower_half, jnp.sin(phase_angle), jnp.cos(phase_angle))


def dot(a, b):
    return jnp.dot(a, b, preferred_element_type=F32)


def iota(shape, dim):
    return lax.broadcasted_iota(jnp.int32, shape, dim)


def one_hot(condition):
    return jnp.where(condition, 1.0, 0.0).astype(BF16)


def kernel(
    nx, nz,
    lat, spec, wv_in, wg_in, wo_in, table, ids, emb, kw, kh, kt,
    out,
    spread, arrived, spin, spout, back, returned, y_own, y_other, filt, gain, total,
    wall, wo_other, mix_own, mix_other, counts, space, wide, narrow,
    a_send, a_recv, b_send, b_recv, s_send, s_recv, r_send, r_recv,
    y_send, y_recv, o_send, o_recv, m_send, m_recv,
):
    n = nx * nz
    rows, chans = lat.shape
    part = wv_in.shape[1]
    lines = rows // WW
    block = rows // n
    mx, mz, core = lax.axis_index("sp_0"), lax.axis_index("sp_1"), lax.axis_index("ch")
    me = mx * nz + mz
    other_core = {"ch": 1 - core}
    tile = rows // nx
    per = tile // block

    def x_step(turn):
        return jnp.where(turn == 0, 2, jnp.where(turn == 1, 1, jnp.where(turn == 2, 3, 0)))

    def partner(i):
        zi = nz - 1 - i % nz
        m = (zi + 1) // 2
        dz = jnp.where(zi % 2 == 1, m, nz - m) % nz
        tx, tz = (mx + x_step(i // nz)) % nx, (mz + dz) % nz
        return {"sp_0": tx, "sp_1": tz}, tx * nz + tz

    def blocks_of(column):
        return pl.ds(pl.multiple_of(column * nz, nz), nz)

    def rows_of(column):
        return pl.ds(pl.multiple_of(column * tile, tile), tile)

    barrier = pltpu.get_barrier_semaphore()

    def greet(i, carry):
        device, _ = partner(i)
        pl.semaphore_signal(barrier, inc=1, device_id=device, device_id_type=MESH)
        return carry

    lax.fori_loop(0, n - 1, greet, 0)
    pl.semaphore_signal(barrier, inc=1, device_id=other_core, device_id_type=MESH)

    pick = one_hot(iota((rows, WW), 0) // lines == iota((rows, WW), 1))
    spread_rows = dot(pick, kw[...]).astype(BF16)
    line_of = iota((rows, WW), 0) % lines
    for line in range(lines):
        narrow[:, line * WW : (line + 1) * WW] = jnp.where(
            line_of == line, spread_rows, jnp.zeros_like(spread_rows)
        )
    mine = pl.ds(pl.multiple_of(core * part, 128), part)

    def widen(r, carry):
        at = pl.ds(pl.multiple_of(r * tile, tile), tile)
        got = dot(narrow[at, :], lat[:, mine]).astype(BF16)
        spread[pl.ds(r * per, per)] = got.reshape(per, block, part)
        return carry

    lax.fori_loop(0, rows // tile, widen, 0)
    arrived[me] = spread[me]
    wall[mx, mz // STRIDE, mz % STRIDE, :, 0:part] = wv_in[...]
    wall[mx, mz // STRIDE, mz % STRIDE, :, part : 2 * part] = wg_in[...]
    wall[mx, mz // STRIDE, mz % STRIDE, :, 2 * part : 3 * part] = wo_in[:, mine]

    pl.semaphore_wait(barrier, n)

    groups = nz // STRIDE
    up = (groups + 1) // 2
    down = groups - 1 - up

    first_part = pl.ds(0, part)
    later_part = pl.ds(part, 2 * part + 128)

    def hop(direction, q):
        origin = (mz // STRIDE - direction * (q - 1) + groups) % groups
        ref = wall.at[mx, origin, mz % STRIDE]
        k = (q - 1) if direction > 0 else up + q - 1
        return pltpu.make_async_remote_copy(
            src_ref=ref, dst_ref=ref, send_sem=s_send.at[k], recv_sem=s_recv.at[k],
            device_id={"sp_1": (mz + direction * STRIDE + nz) % nz}, device_id_type=MESH,
        )

    def hop_in(q):
        hop(1, q).wait_recv()
        if q <= down:
            hop(-1, q).wait_recv()

    def hop_out(q):
        hop(1, q).start()
        if q <= down:
            hop(-1, q).start()

    def group_span(k):
        return ((0, groups), (0, groups), (groups // 2, groups), (0, groups // 2))[k]

    def piece(stage, k, g, count):
        step = (1, -1, 1, -1)[k]
        back_by = (0, 0, 1, -1)[k]
        lanes = (first_part, later_part)[stage // 2]
        if stage % 2:
            ref = wall.at[(mx - back_by + nx) % nx, pl.ds(g, count), :, :, lanes]
            device = {"sp_0": (mx + step + nx) % nx}
        else:
            ref = wall.at[mx, pl.ds(g, count), (mz - back_by + nz) % STRIDE, :, lanes]
            device = {"sp_1": (mz + step + nz) % nz}
        return pltpu.make_async_remote_copy(
            src_ref=ref, dst_ref=ref, send_sem=r_send.at[stage, k], recv_sem=r_recv.at[stage, k],
            device_id=device, device_id_type=MESH,
        )

    def whole(stage, k):
        low, high = group_span(k)
        return piece(stage, k, low, high - low)

    def exchange(src, dst, send_sem, recv_sem):
        def copy(i):
            device, target = partner(i)
            return pltpu.make_async_remote_copy(
                src_ref=src.at[target], dst_ref=dst.at[me],
                send_sem=send_sem.at[i], recv_sem=recv_sem.at[i // nz],
                device_id=device, device_id_type=MESH,
            )

        def send(first, last):
            def body(i, carry):
                @pl.when(i >= WINDOW)
                def _():
                    copy(i - WINDOW).wait_send()

                copy(i).start()
                return carry

            lax.fori_loop(first, last, body, 0)

        def drain():
            def body(i, carry):
                copy(i).wait_send()
                return carry

            lax.fori_loop(n - 1 - WINDOW, n - 1, body, 0)

        def arrive(turn):
            column = (mx - (2, 1, 3, 0)[turn] + nx) % nx
            some = dst.at[pl.ds(column * nz, nz - 1 if turn == nx - 1 else nz)]
            pltpu.make_async_copy(some, some, recv_sem.at[turn]).wait()
            return column

        return send, drain, arrive

    send, drain, arrive = exchange(spread, arrived, a_send, a_recv)
    send(0, 8)

    vocab = table.shape[1]
    low_count = 256
    high_count = vocab // low_count
    prompt = ids.shape[1]
    high_hot = one_hot(ids[...] // low_count == iota((high_count, prompt), 0))
    low_hot = one_hot(ids[...] % low_count == iota((low_count, prompt), 0))
    counts[...] = lax.dot_general(
        high_hot, low_hot, (((1,), (1,)), ((), ())), preferred_element_type=F32
    )

    def tally(h, total):
        piece = table[:, pl.ds(pl.multiple_of(h * low_count, low_count), low_count)]
        return total + piece.astype(F32) * counts[pl.ds(h, 1), :]

    few = table.shape[0]
    tallied = lax.fori_loop(0, high_count, tally, jnp.zeros((few, low_count), F32))
    pooled4 = jnp.sum(tallied, axis=1, keepdims=True) * (1.0 / prompt)
    pooled8 = jnp.concatenate([pooled4] * (block // few), axis=0)
    pooled8 = jnp.where(iota((block, 1), 0) // few == core, pooled8, 0.0)
    first = pooled8.astype(BF16).astype(F32)
    second = (pooled8 - first).astype(BF16).astype(F32)
    third = pooled8 - first - second
    lane = iota((block, 128), 1)
    terms = jnp.where(lane == 0, first, jnp.where(lane == 1, second, jnp.where(lane == 2, third, 0.0)))
    wall[mx, mz // STRIDE, mz % STRIDE, :, 3 * part : 3 * part + 128] = terms.astype(BF16)
    hop_out(1)

    def send_hops(at, pace):
        for q in range(1, up + 1):
            send(at, at + pace)
            at += pace
            hop_in(q)
            if q < up:
                hop_out(q + 1)
        return at

    def send_pieces(stage, at, each, slack):
        for pair in ((0, 1), (2, 3)):
            count = group_span(pair[0])[1] - group_span(pair[0])[0]

            def body(g, carry, at=at, pair=pair):
                for k in pair:
                    piece(stage, k, group_span(k)[0] + g, 1).start()
                send(at + g * each, at + (g + 1) * each)
                return carry

            lax.fori_loop(0, count, body, 0)
            at += count * each
            send(at, at + slack)
            at += slack
            for k in pair:
                whole(stage, k).wait_recv()
        return at

    cells = TT * HH
    kt_wide = dot(kt[...], one_hot(iota((TT, cells), 1) // HH == iota((TT, cells), 0)))
    kh_wide = dot(kh[...], one_hot(iota((HH, cells), 1) % HH == iota((HH, cells), 0)))
    for s in range(TT):
        space[s * HH : (s + 1) * HH, :] = (kh_wide * kt_wide[s : s + 1, :]).astype(BF16)
    kw_wide = dot(kw[...], one_hot(iota((WW, rows), 1) // lines == iota((WW, rows), 0)))
    column_line = iota((WW, rows), 1) % lines
    for line in range(lines):
        wide[line * WW : (line + 1) * WW, :] = jnp.where(column_line == line, kw_wide, 0.0).astype(BF16)
    at = send_hops(8, 13)
    at = send_pieces(0, at, 1, 8)
    at = send_pieces(1, at, 1, 8)
    send(at, n - 1)
    for turn in range(nx - 1):
        column = arrive(turn)
        for r in range(nx):
            here = slice(r * tile, (r + 1) * tile)
            got = dot(space[here, rows_of(column)], arrived[blocks_of(column)].reshape(tile, part))
            total[here, :] = got if turn == 0 else total[here, :] + got
    drain()
    column = arrive(nx - 1)

    quarters = rows // tile
    gathered = wall.reshape(chans, 3 * part + 128)
    value_weight = gathered.at[:, 0:part]
    own_rows = pl.ds(pl.multiple_of(core * part, part), part)
    other_rows = pl.ds(pl.multiple_of((1 - core) * part, part), part)
    ycopies = [
        pltpu.make_async_remote_copy(
            src_ref=y_own.at[pl.ds(r * tile, tile)], dst_ref=y_other.at[pl.ds(r * tile, tile)],
            send_sem=y_send.at[r], recv_sem=y_recv.at[r], device_id=other_core, device_id_type=MESH,
        )
        for r in range(quarters)
    ]

    def forward(r):
        here = slice(r * tile, (r + 1) * tile)
        got = dot(space[here, rows_of(column)], arrived[blocks_of(column)].reshape(tile, part))
        y_own[here, :] = (total[here, :] + got).astype(BF16)
        ycopies[r].start()

    def project(r):
        here = slice(r * tile, (r + 1) * tile)
        ycopies[r].wait_recv()
        value = dot(y_own[here, :], value_weight[own_rows, :])
        value = value + dot(y_other[here, :], value_weight[other_rows, :])
        filt[here, :] = (value * spec[here, :].astype(F32)).astype(BF16)

    def backward(turn):
        target = (mx + (2, 1, 3, 0)[turn]) % nx
        got = dot(space[rows_of(target), :], filt[...]).astype(BF16)
        back[blocks_of(target)] = got.reshape(per, block, part)

    whole(2, 0).start()
    whole(2, 1).start()
    for r in range(nx):
        forward(r)
    for r in range(nx):
        project(r)
    whole(2, 0).wait_recv()
    whole(2, 1).wait_recv()
    whole(2, 2).start()
    whole(2, 3).start()
    send, drain, arrive = exchange(back, returned, b_send, b_recv)
    backward(0)
    send(0, nz // 2)
    backward(1)
    send(nz // 2, nz)
    for turn in range(2, nx):
        backward(turn)
    returned[me] = back[me]
    for r in range(nx):
        ycopies[r].wait_send()
    whole(2, 2).wait_recv()
    whole(2, 3).wait_recv()
    at = send_pieces(3, nz, 4, 16)
    send(at, n - 1)
    for q in range(1, up + 1):
        hop(1, q).wait_send()
        if q <= down:
            hop(-1, q).wait_send()
    for stage in range(4):
        for k in range(4):
            whole(stage, k).wait_send()

    upper = pl.ds(2 * part, part + 128)
    swap_out = pltpu.make_async_remote_copy(
        src_ref=wall.at[:, :, :, :, upper], dst_ref=wo_other, send_sem=o_send, recv_sem=o_recv,
        device_id=other_core, device_id_type=MESH,
    )
    swap_out.start()
    swap_out.wait()
    others = wo_other.reshape(chans, part + 128)
    pools = gathered[:, 3 * part : 3 * part + 128] + others[:, part : part + 128]
    chosen = one_hot(iota((chans, part), 0) == iota((chans, part), 1) + core * part)
    terms = lax.dot_general(pools, chosen, (((0,), (0,)), ((), ())), preferred_element_type=F32)
    modulation = 1.0 + jnp.sum(terms[0:8, :], axis=0, keepdims=True) + emb[...]

    def gate(r, carry):
        here = pl.ds(pl.multiple_of(r * tile, tile), tile)
        v = dot(lat[here, :], gathered[:, part : 2 * part])
        gain[here, :] = v / (1.0 + jnp.exp(-v)) * modulation
        return carry

    lax.fori_loop(0, quarters, gate, 0)
    for turn in range(nx - 1):
        column = arrive(turn)
        for r in range(nx):
            here = slice(r * tile, (r + 1) * tile)
            got = dot(wide[here, rows_of(column)], returned[blocks_of(column)].reshape(tile, part))
            total[here, :] = got if turn == 0 else total[here, :] + got
    drain()
    last = arrive(nx - 1)

    half = rows // 2

    def finish(r, dst, base):
        here = pl.ds(pl.multiple_of(base + r * tile, tile), tile)
        mix = dot(wide[here, rows_of(last)], returned[blocks_of(last)].reshape(tile, part))
        mix = (total[here, :] + mix) * gain[here, :]
        dst[pl.ds(pl.multiple_of(r * tile, tile), tile), :] = mix.astype(BF16)

    mcopies = []
    for r in range(half // tile):
        finish(r, spout, (1 - core) * half)
        mcopies.append(pltpu.make_async_remote_copy(
            src_ref=spout.at[pl.ds(r * tile, tile)], dst_ref=mix_other.at[pl.ds(r * tile, tile)],
            send_sem=m_send.at[r], recv_sem=m_recv.at[r], device_id=other_core, device_id_type=MESH,
        ))
        mcopies[-1].start()
    for r in range(half // tile):
        finish(r, mix_own, core * half)
    left = pl.ds(pl.multiple_of(core * part, part), part)
    right = pl.ds(pl.multiple_of((1 - core) * part, part), part)
    for r in range(half // tile):
        here = slice(r * tile, (r + 1) * tile)
        mcopies[r].wait()
        own_cells = pl.ds(pl.multiple_of(core * half + r * tile, tile), tile)
        for at, weight in ((left, gathered.at[:, 2 * part : 3 * part]), (right, others.at[:, 0:part])):
            added = dot(mix_own[here, :], weight[own_rows, :]) + dot(
                mix_other[here, :], weight[other_rows, :]
            )
            out[here, at] = (lat[own_cells, at].astype(F32) + added).astype(BF16)


def local(nx, nz, latents, spectrum, w_value, w_gate, w_out, embed_table, prompt_ids, noise_step):
    rows, chans = latents.shape
    block, part = w_value.shape
    n = nx * nz
    core = lax.axis_index("ch")
    channel = core * part + jnp.arange(part, dtype=jnp.int32)
    emb = step_embedding(noise_step, channel, chans).reshape(1, part)
    half = rows // 2
    groups = nz // STRIDE
    hops = groups - 1
    vmem = pl.BlockSpec(memory_space=pltpu.VMEM)
    dma = pltpu.SemaphoreType.DMA
    exchanged = pltpu.VMEM((n, rows // n, part), BF16)
    plain = pltpu.VMEM((rows, part), BF16)
    return pl.pallas_call(
        functools.partial(kernel, nx, nz),
        out_shape=jax.ShapeDtypeStruct((half, chans), BF16),
        in_specs=[vmem] * 11,
        out_specs=vmem,
        scratch_shapes=[
            exchanged, exchanged,
            pltpu.VMEM((8, 128), BF16), pltpu.VMEM((half, part), BF16),
            exchanged, exchanged,
            plain, plain, plain,
            pltpu.VMEM((rows, part), F32), pltpu.VMEM((rows, part), F32),
            pltpu.VMEM((nx, groups, STRIDE, block, 3 * part + 128), BF16),
            pltpu.VMEM((nx, groups, STRIDE, block, part + 128), BF16),
            pltpu.VMEM((half, part), BF16), pltpu.VMEM((half, part), BF16),
            pltpu.VMEM((embed_table.shape[1] // 256, 256), F32),
            pltpu.VMEM((rows, rows), BF16), pltpu.VMEM((rows, rows), BF16), pltpu.VMEM((rows, rows), BF16),
            dma((n,)), dma((nx,)), dma((n,)), dma((nx,)),
            dma((hops,)), dma((hops,)), dma((4, 4)), dma((4, 4)),
            dma((4,)), dma((4,)), dma, dma, dma((2,)), dma((2,)),
        ],
        compiler_params=pltpu.CompilerParams(
            collective_id=0, has_side_effects=True, vmem_limit_bytes=56 * 2**20
        ),
    )(
        latents, spectrum.reshape(rows, part), w_value, w_gate, w_out, embed_table,
        prompt_ids.reshape(1, -1), emb, cas_table(WW), cas_table(HH), cas_table(TT),
    )


def solution(mesh):
    nx, nz = 4, mesh.shape["sp"] // 4
    torus = Mesh(
        mesh.devices.reshape(mesh.shape["grp"], nx, nz, mesh.shape["ch"]),
        ("grp", "sp_0", "sp_1", "ch"),
    )
    in_specs = (
        P(GRP_SP, None),
        P(None, None, SP, "ch"),
        P(SP, "ch"),
        P(SP, "ch"),
        P(SP, None),
        P(SP_CH, None),
        P("grp"),
        P("grp"),
    )
    out_specs = P(GRP_SP_CH, None)
    return jax.shard_map(
        functools.partial(local, nx, nz),
        mesh=torus, in_specs=in_specs, out_specs=out_specs, check_vma=False,
    )
```
